128 devices in a mesh: batch: 1, row: 16 (over z, y), col: 8 (over x, core).
Axes of the slice: x: 4, y: 4, z: 4, core: 2. Of those that a mesh axis runs over, the one named last changes fastest.
Arguments:
- lower_tri: bfloat16 [16384, 16384], P(('batch', 'row'), 'col')
- right_side: bfloat16 [16384, 4096], P(('batch', 'row'), 'col')
- grad_out: bfloat16 [16384, 4096], P(('batch', 'row'), 'col')
Outputs:
- output 1: bfloat16 [16384, 4096], P(('batch', 'row'), 'col')
- output 2: bfloat16 [16384, 16384], P(('batch', 'row'), 'col')
All inputs are finite; a program needn't handle non-finite values.
Results may differ from the reference program's by a relative error of at most 0.001.
Values are sent between devices in bfloat16 or wider.
A program may use at most 1 GiB of HBM per device.

```python
import jax
import jax.numpy as jnp

MAT_ORDER = 16384
BLOCK_SIZE = 256
RHS_COLS = 4096
MESH_ROWS = 16
MESH_COLS = 8
ROW_BLOCKS = MAT_ORDER // (BLOCK_SIZE * MESH_ROWS)
COL_BLOCKS = MAT_ORDER // (BLOCK_SIZE * MESH_COLS)


def rows_to_global(stored):
    num_cols = stored.shape[1]
    return stored.reshape(MESH_ROWS, ROW_BLOCKS, BLOCK_SIZE, num_cols).transpose(1, 0, 2, 3).reshape(MAT_ORDER, num_cols)


def rows_to_stored(natural):
    num_cols = natural.shape[1]
    return natural.reshape(ROW_BLOCKS, MESH_ROWS, BLOCK_SIZE, num_cols).transpose(1, 0, 2, 3).reshape(MAT_ORDER, num_cols)


def cols_to_global(stored):
    num_rows = stored.shape[0]
    return stored.reshape(num_rows, MESH_COLS, COL_BLOCKS, BLOCK_SIZE).transpose(0, 2, 1, 3).reshape(num_rows, MAT_ORDER)


def cols_to_stored(natural):
    num_rows = natural.shape[0]
    return natural.reshape(num_rows, COL_BLOCKS, MESH_COLS, BLOCK_SIZE).transpose(0, 2, 1, 3).reshape(num_rows, MAT_ORDER)


def setup_inputs(seed: int = 0, part: int = 0) -> dict:
    base_key = jax.random.fold_in(jax.random.key(seed), part)
    key_lower, key_right, key_grad = jax.random.split(base_key, 3)
    lower_mat = jax.random.normal(key_lower, (MAT_ORDER, MAT_ORDER), jnp.float32) * (MAT_ORDER ** -0.5)
    lower_mat = jnp.tril(lower_mat).astype(jnp.bfloat16)
    right_mat = jax.random.normal(key_right, (MAT_ORDER, RHS_COLS), jnp.float32) * (RHS_COLS ** -0.5)
    grad_mat = jax.random.normal(key_grad, (MAT_ORDER, RHS_COLS), jnp.float32)
    return {
        "lower_tri": cols_to_stored(rows_to_stored(lower_mat)),
        "right_side": rows_to_stored(right_mat.astype(jnp.bfloat16)),
        "grad_out": rows_to_stored(grad_mat.astype(jnp.bfloat16)),
    }


def reference(lower_tri, right_side, grad_out):
    lower_mat = cols_to_global(rows_to_global(lower_tri))
    right_mat = rows_to_global(right_side)
    grad_mat = rows_to_global(grad_out)
    grad_right = jnp.dot(lower_mat.T, grad_mat, preferred_element_type=jnp.float32)
    grad_lower = jnp.tril(jnp.dot(grad_mat, right_mat.T, preferred_element_type=jnp.float32))
    return (rows_to_stored(grad_right.astype(jnp.bfloat16)), cols_to_stored(rows_to_stored(grad_lower.astype(jnp.bfloat16))))
```

```python
import heapq

import jax
import jax.numpy as jnp
from jax import lax
from jax.experimental import pallas as pl
from jax.experimental.pallas import tpu as pltpu
from jax.sharding import PartitionSpec as P

BLOCK = 256
MESH = pl.DeviceIdType.MESH
L_RUNS = (((0, 0, 3), (1, 1, 1)), ((1, 2, 3), (2, 2, 3), (3, 3, 3)))


def plan():
    jobs = {}
    for name, first in (("grad", 0), ("side", 1)):
        def hop(off, axis, step):
            moved = list(off)
            moved[axis] = (moved[axis] - step) % 4
            return tuple(moved)
        for half in range(2):
            for lane in [None, 0, 1, 2, 3]:
                axis = first if lane is None else 1 - first
                own = [0, 0]
                if lane is not None:
                    own[first] = lane
                own = tuple(own)
                for step in (1, -1):
                    jobs[(name, own, half, axis, step)] = ((name, own, half), (axis, step), 11.3, (name, hop(own, axis, step), half))
                step = 1 if half == 0 else -1
                near = hop(own, axis, step)
                jobs[(name, near, half, axis, step)] = ((name, near, half), (axis, step), 11.3, (name, hop(near, axis, step), half))
    for name, pieces, cost in (("line", 1, 11.3), ("low", 2, 14.1)):
        for q in range(pieces):
            for half in range(2):
                for step in (1, -1):
                    jobs[(name, (0, 0, q), half, 2, step)] = ((name, (0, 0, q), half), (2, step), cost, (name, (-step % 4, 0, q), half))
                step = 1 if half == 0 else -1
                jobs[(name, (-step % 4, 0, q), half, 2, step)] = ((name, (-step % 4, 0, q), half), (2, step), cost, (name, (2, 0, q), half))
                for off in range(4):
                    jobs[(name, (off, 0, q), half, 3, 1)] = ((name, (off, 0, q), half), (3, 1), cost / 8, (name, (off, 1, q), half))
    ready = {}
    for half in range(2):
        ready[("grad", (0, 0), half)] = 0.0
        ready[("line", (0, 0, 0), half)] = 0.0
        ready[("side", (0, 0), half)] = 30.0
        for q in range(2):
            ready[("low", (0, 0, q), half)] = 50.0 + 10 * q
    waiting = dict(jobs)
    free = {}
    order = []
    while waiting:
        best = None
        for key, (need, link, cost, made) in waiting.items():
            if need in ready:
                start = max(ready[need], free.get(link, 0.0))
                rank = (start, ready[need], str(key))
                if best is None or rank < best[0]:
                    best = (rank, key)
        (start, avail, _), key = best
        need, link, cost, made = waiting.pop(key)
        free[link] = start + cost
        assert made not in ready
        ready[made] = start + cost + 2.5
        order.append((max(avail, start - 12.0), start, key))
    order.sort(key=lambda t: (t[0], t[1]))
    ends = sorted((t, e) for e, t in ready.items())
    return jobs, [key for _, _, key in order], ends


def gather_kernel(low_ref, side_ref, grad_ref, low_all, side_all, grad_all, line_all, stage,
                  low_recv, side_recv, grad_recv, line_recv, send_sem, local_sem):
    r, c = lax.axis_index("row"), lax.axis_index("col")
    z, y, x, core = r // 4, r % 4, c // 2, c % 2

    def place(zz, yy, xx, cc):
        return {"row": zz * 4 + yy, "col": xx * 2 + cc}

    def low_slot(xx, cc, q):
        h = r // 8
        dx = (xx + 4 - (r % 8) // 2) % 4
        dc = (cc + r) % 2
        yy = (dx + h * (4 - 2 * dx)) % 4
        zz = 2 - 2 * h + dc * (4 * h - 2) + q
        return zz * 4 + yy

    def slot(name, off):
        if name in ("grad", "side"):
            return ((z + off[0]) % 4) * 4 + (y + off[1]) % 4
        xx, cc = (x + off[0]) % 4, (core + off[1]) % 2
        if name == "line":
            return xx * 2 + 1 - cc
        return low_slot(xx, cc, off[2])

    bufs = {"grad": (grad_all, grad_recv, 0), "side": (side_all, side_recv, 1),
            "line": (line_all, line_recv, 2), "low": (low_all, low_recv, 3)}

    def local(src, dst, i):
        return pltpu.make_async_copy(src, dst, local_sem.at[i])

    side_row = (r // 8) * 8 + c + 1 - 2 * (c % 2)
    pltpu.make_async_remote_copy(side_ref, side_all.at[side_row], send_sem.at[1], side_recv.at[side_row, 0],
                                 device_id={"row": side_row, "col": r % 8}, device_id_type=MESH).start()

    def send_low():
        for h in range(2):
            xx = (x + (y if h == 0 else 4 - y)) % 4
            same = (z // 2) if h == 1 else 1 - z // 2
            dest = {"row": c + 8 * h, "col": xx * 2 + (core + same) % 2}
            for half in range(2):
                at = 0
                for kb, b0, b1 in L_RUNS[half]:
                    n = (b1 + 1 - b0) * BLOCK
                    pltpu.make_async_remote_copy(
                        low_ref.at[pl.ds(b0 * BLOCK, n), pl.ds((2 * kb + h) * BLOCK, BLOCK)],
                        low_all.at[r, half, pl.ds(at, n)], send_sem.at[3], low_recv.at[r, half],
                        device_id=dest, device_id_type=MESH).start()
                    at += n

    local(grad_ref, stage, 0).start()
    jobs, order, ends = plan()
    waited = set()

    def wait(event):
        if event in waited:
            return
        waited.add(event)
        name, off, half = event
        buf, recv, _ = bufs[name]
        s = slot(name, off)
        if name == "side" and off == (0, 0):
            waited.add((name, off, 1 - half))
            pltpu.make_async_copy(buf.at[s], buf.at[s], recv.at[s, 0]).wait()
            return
        pltpu.make_async_copy(buf.at[s, half], buf.at[s, half], recv.at[s, half]).wait()

    own = {("grad", (0, 0)), ("line", (0, 0, 0))}
    sent_low = False
    for key in order:
        name, off, half, axis, step = key
        buf, recv, i = bufs[name]
        if (name, off) in own:
            src = grad_ref.at[half]
        else:
            if not sent_low:
                send_low()
                sent_low = True
                local(grad_ref, stage, 0).wait()
                local(stage, grad_all.at[slot("grad", (0, 0))], 1).start()
                local(stage, line_all.at[slot("line", (0, 0, 0))], 2).start()
            wait((name, off, half))
            src = buf.at[slot(name, off), half]
        to = [z, y, x, core]
        to[axis] = (to[axis] + step + 4) % 4 if axis < 3 else 1 - core
        s = slot(name, off)
        pltpu.make_async_remote_copy(src, buf.at[s, half], send_sem.at[i], recv.at[s, half],
                                     device_id=place(*to), device_id_type=MESH).start()
    for _, event in ends:
        if event[:2] not in own:
            wait(event)
    local(stage, grad_all.at[slot("grad", (0, 0))], 1).wait()
    local(stage, line_all.at[slot("line", (0, 0, 0))], 2).wait()
    for i, part in ((0, grad_all.at[pl.ds(0, 15)]), (1, side_all), (2, line_all.at[pl.ds(0, 7)]), (3, low_all)):
        pltpu.make_async_copy(part, part, send_sem.at[i]).wait()


def gather(low, side, grad):
    cols = side.shape[1]
    half = (2, 2 * BLOCK, cols)
    piece = (2, 5 * BLOCK, BLOCK)
    dt = low.dtype
    anywhere = pl.BlockSpec(memory_space=pl.ANY)
    return pl.pallas_call(
        gather_kernel,
        out_shape=[jax.ShapeDtypeStruct((16, *piece), dt), jax.ShapeDtypeStruct((16, *half), dt),
                   jax.ShapeDtypeStruct((16, *half), dt), jax.ShapeDtypeStruct((8, *half), dt)],
        in_specs=[anywhere] * 3,
        out_specs=[anywhere] * 4,
        scratch_shapes=[
            pltpu.VMEM(half, dt),
            pltpu.SemaphoreType.DMA((16, 2)),
            pltpu.SemaphoreType.DMA((16, 2)),
            pltpu.SemaphoreType.DMA((16, 2)),
            pltpu.SemaphoreType.DMA((8, 2)),
            pltpu.SemaphoreType.DMA((4,)),
            pltpu.SemaphoreType.DMA((3,)),
        ],
        compiler_params=pltpu.CompilerParams(has_side_effects=True),
        name="gather",
    )(low, side.reshape(half), grad.reshape(half))


def products(low_all, side_all, grad_all, line_all):
    cols = side_all.shape[-1]
    low = low_all.reshape(16, 10, BLOCK, BLOCK)
    grad = grad_all.reshape(16, 4, BLOCK, cols)
    first = (0, 4, 7, 9)
    right = []
    for kb in range(4):
        n = 4 - kb
        right.append(jnp.einsum("rbik,rbij->kj", low[:, first[kb]:first[kb] + n], grad[:, kb:],
                                preferred_element_type=jnp.float32).astype(jnp.bfloat16))
    line = line_all.reshape(8, 4, BLOCK, cols)
    side = side_all.reshape(2, 8, 4, BLOCK, cols)
    lower = []
    for bi in range(4):
        part = jnp.einsum("sif,hskef->ikhe", line[:, bi], side[:, :, :bi + 1], preferred_element_type=jnp.float32)
        part = part.astype(jnp.bfloat16).reshape(BLOCK, (bi + 1) * 2 * BLOCK)
        lower.append(jnp.pad(part, ((0, 0), (0, (3 - bi) * 2 * BLOCK))))
    return jnp.concatenate(right, 0), jnp.concatenate(lower, 0)


def per_device(low, side, grad):
    right, lower = products(*gather(low, side, grad))
    rows_here, cols_here = lower.shape
    row_pos = jnp.arange(rows_here)[:, None]
    col_pos = jnp.arange(cols_here)[None, :]
    row_global = (row_pos // BLOCK * 16 + lax.axis_index("row")) * BLOCK + row_pos % BLOCK
    col_global = (col_pos // BLOCK * 8 + lax.axis_index("col")) * BLOCK + col_pos % BLOCK
    return right, jnp.where(row_global >= col_global, lower, jnp.zeros_like(lower))


def solution(mesh):
    spec = P(("batch", "row"), "col")
    return jax.shard_map(per_device, mesh=mesh, in_specs=(spec,) * 3, out_specs=(spec,) * 2, check_vma=False)
```

```python
import jax
import jax.numpy as jnp
from jax import lax
from jax.experimental import pallas as pl
from jax.experimental.pallas import tpu as pltpu
from jax.sharding import PartitionSpec as P

BLOCK = 256
MESH = pl.DeviceIdType.MESH
NROWS = (1024, 768, 512, 256)
FIRST = (0, 1024, 1792, 2304)
LAG = 2.5


def plan():
    ready, jobs, steps = {}, [], []

    def job(need, link, cost, made, prio, step):
        jobs.append((need, link, cost, made, prio, step))

    for q in range(4):
        first = 1 if q < 2 else 0
        def hop(off, axis, d):
            moved = list(off)
            moved[axis] = (moved[axis] - d) % 4
            return tuple(moved)
        ready[("side", (0, 0), q)] = 24.0
        for lane in (None, 0, 1, 3, 2):
            axis = first if lane is None else 1 - first
            own = [0, 0]
            if lane is not None:
                own[first] = lane
            own = tuple(own)
            prio = 1 if lane is None else 5
            for d in (1, -1):
                job(("side", own, q), ("zy"[axis], d), 5.65, ("side", hop(own, axis, d), q), prio, ("side", own, q, axis, d))
            d = 1 if q % 2 == 0 else -1
            near = hop(own, axis, d)
            job(("side", near, q), ("zy"[axis], d), 5.65, ("side", hop(near, axis, d), q), prio, ("side", near, q, axis, d))
    for half in range(2):
        ready[("grad", 0, half)] = 0.0
        ready[("line", "own", half)] = 0.0
        for d in (1, -1):
            job(("grad", 0, half), ("z", d), 11.3, ("grad", -d % 4, half), 3, ("grad", 0, half, d))
        d = 1 if half == 0 else -1
        job(("grad", -d % 4, half), ("z", d), 11.3, ("grad", 2, half), 3, ("grad", -d % 4, half, d))
        for to in "ab":
            job(("line", "own", half), to, 11.3, ("line", to, half), 4, ("line", "own", half, to))
        src, to = ("a", "b") if half == 0 else ("b", "a")
        job(("line", src, half), to, 11.3, ("line", "o", half), 4, ("line", src, half, to))
        for piece in ("own", "a", "b", "o"):
            job(("line", piece, half), "sib", 1.0, ("line", piece + "s", half), 4, ("line", piece, half, "sib"))
    done = 2.0
    for kb in range(4):
        cost = 11.3 * NROWS[kb] / 1024
        done += 1.5 * cost
        for zz in range(4):
            ready[("hub", kb, zz)] = done
            job(("hub", kb, zz), "b", cost, ("p", kb, zz), 2, ("hub", kb, zz))
            job(("p", kb, zz), "a", cost, ("q", kb, zz), 2, ("p", kb, zz))
            job(("q", kb, zz), "sib", 0.1 * cost, ("qs", kb, zz), 2, ("q", kb, zz))
    free = {("z", 1): 20.0, ("z", -1): 20.0}
    pending = list(jobs)
    while pending:
        best = min((j for j in pending if j[0] in ready),
                   key=lambda j: (max(ready[j[0]], free.get(j[1], 0.0)), j[4], ready[j[0]]))
        pending.remove(best)
        need, link, cost, made, prio, step = best
        start = max(ready[need], free.get(link, 0.0))
        free[link] = start + cost
        ready[made] = start + cost + LAG
        steps.append((max(ready[need], start - 12.0), start, ("send",) + step))
        for kb in range(4):
            key = ("sum", kb)
            if key not in ready and all(("qs", kb, zz) in ready for zz in range(4)):
                now = max(ready[("qs", kb, zz)] for zz in range(4)) + 3.0
                ready[key] = now
                steps.append((now, now, ("part", kb)))
                for d in (1, -1):
                    pending.append((key, ("y", d), 5.65, ("hop", kb, d), 0, ("far", kb, d)))
                    pending.append((("hop", kb, d), ("y", d), 11.3, ("got", kb, d), 0, ("near", kb, d)))
    slots = sorted((max(ready[("side", (a, b), q)] for q in range(4)), (a, b)) for a in range(4) for b in range(4))
    for g in range(4):
        now = max(max(t for t, _ in slots[4 * g:4 * g + 4]), max(t for e, t in ready.items() if e[0] == "line")) + 1.0
        steps.append((now, now, ("dot", tuple(off for _, off in slots[4 * g:4 * g + 4]))))
    steps.sort(key=lambda t: (t[0], t[1]))
    return [s for _, _, s in steps], ready


def kernel(low_ref, side_ref, grad_ref, right_ref, lower_ref, low_all,
           side_all, grad_all, line_all, acc, part, hop, got, lbuf, stage, obuf, rbuf,
           low_recv, side_recv, grad_recv, line_recv, hop_recv, got_recv, send_sem, lbuf_sem, stage_sem, out_sem):
    r, c = lax.axis_index("row"), lax.axis_index("col")
    z, y, x, core = r // 4, r % 4, c // 2, c % 2
    hub = x // 2 == z % 2
    xa, xb = x + 1 - 2 * (x % 2), 3 - x
    xh = jnp.where(hub, x, xb)

    def bxor(a, b):
        return sum(((a // n % 2 + b // n % 2) % 2) * n for n in (1, 2, 4))

    def place(zz, yy, xx, cc):
        return {"row": zz * 4 + yy, "col": xx * 2 + cc}

    def remote(src, dst, send, recv, to):
        return pltpu.make_async_remote_copy(src, dst, send_sem.at[send], recv, device_id=to, device_id_type=MESH)

    def arrive(ref, sem):
        pltpu.make_async_copy(ref, ref, sem).wait()

    sib = place(z, y, x, 1 - core)
    up, down = place(z, (y + 1) % 4, x, core), place(z, (y + 3) % 4, x, core)

    side_row = (r // 8) * 8 + bxor(c, r % 8)
    side_self = (side_row == r) & (c == r % 8)
    for q in range(4):
        @pl.when(jnp.logical_not(side_self))
        def _():
            remote(side_ref.at[q], side_all.at[side_row, pl.ds(q * BLOCK, BLOCK)], 0, side_recv.at[side_row, q],
                   {"row": side_row, "col": r % 8}).start()

        @pl.when(side_self)
        def _():
            pltpu.make_async_copy(side_ref.at[q], side_all.at[side_row, pl.ds(q * BLOCK, BLOCK)], side_recv.at[side_row, q]).start()

    mine = 2 * (x % 2) + core

    def low_piece(h, kb):
        return low_ref.at[pl.ds(kb * BLOCK, NROWS[kb]), pl.ds(pl.multiple_of((2 * kb + h) * BLOCK, BLOCK), BLOCK)]

    def low_at(yy, zz, kb):
        return low_all.at[yy, zz, pl.ds(FIRST[kb], NROWS[kb])]

    def stage_at(kb):
        return stage.at[pl.ds(FIRST[kb], NROWS[kb])]

    here = z // 2

    @pl.when(hub)
    def _():
        for kb in range(4):
            pltpu.make_async_copy(low_piece(here, kb), stage_at(kb), stage_sem.at[kb]).start()
            remote(low_piece(1 - here, kb), low_at(mine, z, kb), 1, low_recv.at[mine, z, kb],
                   place((z + 2) % 4, y, x, core)).start()

    @pl.when(jnp.logical_not(hub))
    def _():
        for kb in range(4):
            for h in range(2):
                remote(low_piece(h, kb), low_at(mine, z, kb), 1, low_recv.at[mine, z, kb],
                       place(x // 2 + 2 * h, y, x, core)).start()

    own_grad = pltpu.make_async_copy(grad_ref, grad_all.at[z], out_sem.at[0])
    own_line = pltpu.make_async_copy(grad_ref, line_all.at[c], out_sem.at[1])
    own_grad.start()
    own_line.start()

    @pl.when(hub)
    def _():
        for kb in range(4):
            pltpu.make_async_copy(low_piece(here, kb), stage_at(kb), stage_sem.at[kb]).wait()
            pltpu.make_async_copy(stage_at(kb), low_at(mine, z, kb), low_recv.at[mine, z, kb]).start()

    steps, ready = plan()
    waited = set()

    def line_slot(piece):
        xx = {"own": x, "a": xa, "b": xb, "o": (x + 2) % 4}[piece.rstrip("s")]
        return xx * 2 + (1 - core if piece.endswith("s") else core)

    def half_at(ref, slot, half):
        return ref.at[slot, pl.ds(half * 512, 512)]

    def wait(event):
        if event in waited:
            return
        waited.add(event)
        name = event[0]
        if name == "side":
            slot = ((z + event[1][0]) % 4) * 4 + (y + event[1][1]) % 4
            arrive(side_all.at[slot, pl.ds(event[2] * BLOCK, BLOCK)], side_recv.at[slot, event[2]])
        elif name == "grad":
            slot = (z + event[1]) % 4
            arrive(half_at(grad_all, slot, event[2]), grad_recv.at[slot, event[2]])
        elif name == "line":
            slot = line_slot(event[1])
            arrive(half_at(line_all, slot, event[2]), line_recv.at[slot, event[2]])
        else:
            yy = 2 * (xh % 2 if name in ("p", "ps") else 1 - xh % 2) + (1 - core if name.endswith("s") else core)
            arrive(low_at(yy, event[2], event[1]), low_recv.at[yy, event[2], event[1]])

    def low_send(yy, zz, kb, send, to):
        remote(low_at(yy, zz, kb), low_at(yy, zz, kb), send, low_recv.at[yy, zz, kb], to).start()

    def send(step):
        name = step[0]
        if name == "side":
            _, off, q, axis, d = step
            wait(("side", off, q))
            slot = ((z + off[0]) % 4) * 4 + (y + off[1]) % 4
            to = place((z + d + 4) % 4, y, x, core) if axis == 0 else place(z, (y + d + 4) % 4, x, core)
            ref = side_all.at[slot, pl.ds(q * BLOCK, BLOCK)]
            remote(ref, ref, 2, side_recv.at[slot, q], to).start()
        elif name == "grad":
            _, off, half, d = step
            if off:
                wait(("grad", off, half))
            slot = (z + off) % 4
            src = half_at(grad_all, slot, half) if off else grad_ref.at[pl.ds(half * 512, 512)]
            remote(src, half_at(grad_all, slot, half), 3, grad_recv.at[slot, half], place((z + d + 4) % 4, y, x, core)).start()
        elif name == "line":
            _, piece, half, to = step
            if piece != "own":
                wait(("line", piece, half))
            slot = line_slot(piece)
            src = half_at(line_all, slot, half) if piece != "own" else grad_ref.at[pl.ds(half * 512, 512)]
            dest = {"a": place(z, y, xa, core), "b": place(z, y, xb, core), "sib": sib}[to]
            remote(src, half_at(line_all, slot, half), 4, line_recv.at[slot, half], dest).start()
        elif name == "hub":
            _, kb, zz = step

            @pl.when(hub)
            def _():
                yy = mine
                arrive(low_at(yy, zz, kb), low_recv.at[yy, zz, kb])
                low_send(yy, zz, kb, 5, place(z, y, xb, core))
                low_send(yy, zz, kb, 5, place(z, y, xa, core))
                low_send(yy, zz, kb, 6, sib)
        elif name == "p":
            _, kb, zz = step
            yy = 2 * (xb % 2) + core

            @pl.when(jnp.logical_not(hub))
            def _():
                arrive(low_at(yy, zz, kb), low_recv.at[yy, zz, kb])
                low_send(yy, zz, kb, 5, place(z, y, xa, core))
                low_send(yy, zz, kb, 6, sib)
        elif name == "q":
            _, kb, zz = step
            wait(("q", kb, zz))
            low_send(2 * (1 - xh % 2) + core, zz, kb, 6, sib)
        elif name == "far":
            _, kb, d = step
            i = 0 if d == 1 else 1
            rows = pl.ds(i * 128, 128)
            remote(part.at[kb, 0, rows], hop.at[kb, i], 7, hop_recv.at[kb, i], up if d == 1 else down).start()
        elif name == "near":
            _, kb, d = step
            i, t = (0, 3) if d == 1 else (1, 1)
            arrive(hop.at[kb, i], hop_recv.at[kb, i])
            rows = pl.ds(i * 128, 128)
            part[kb, t, rows] += hop[kb, i]
            remote(part.at[kb, t], got.at[kb, i], 8, got_recv.at[kb, i], up if d == 1 else down).start()

    def add_part(kb):
        for zz in range(4):
            for name in ("ps", "q", "qs"):
                wait((name, kb, zz))
        if kb == 0:
            own_grad.wait()
            for off in (1, 2, 3):
                for half in range(2):
                    wait(("grad", off, half))
        n = NROWS[kb]

        def load(t):
            return pltpu.make_async_copy(low_all.at[(y + 2 + t) % 4, :, pl.ds(FIRST[kb], n)],
                                         lbuf.at[t % 2, :, pl.ds(0, n)], lbuf_sem.at[t % 2])

        load(0).start()

        def body(t, carry):
            @pl.when(t < 3)
            def _():
                load(t + 1).start()
            load(t).wait()
            total = jnp.zeros((BLOCK, 512), jnp.float32)
            for zz in range(4):
                total += lax.dot_general(lbuf[t % 2, zz, pl.ds(0, n)], grad_all[zz, pl.ds(kb * BLOCK, n)],
                                         (((0,), (0,)), ((), ())), preferred_element_type=jnp.float32)
            part[kb, t] = total
            return carry

        lax.fori_loop(0, 4, body, 0)

    def add_dot(offs, start):
        if start:
            own_line.wait()
            for piece in ("a", "b", "o", "owns", "as", "bs", "os"):
                for half in range(2):
                    wait(("line", piece, half))
            acc[...] = jnp.zeros_like(acc)
        slots = []
        for off in offs:
            for q in range(4):
                wait(("side", off, q))
            slots.append(((z + off[0]) % 4) * 4 + (y + off[1]) % 4)

        def body(i, carry):
            slot = slots[3]
            for n in range(3):
                slot = jnp.where(i == n, slots[n], slot)
            h, cj = slot // 8, bxor(slot % 8, c)
            for bi in range(4):
                n = (bi + 1) * BLOCK
                acc[h, bi, :, :n] += lax.dot_general(
                    line_all[cj, bi * BLOCK:(bi + 1) * BLOCK], side_all[slot, :n],
                    (((1,), (1,)), ((), ())), preferred_element_type=jnp.float32)
            return carry

        lax.fori_loop(0, 4, body, 0)

    started = False
    for step in steps:
        if step[0] == "send":
            send(step[1:])
        elif step[0] == "part":
            add_part(step[1])
        else:
            add_dot(step[1], not started)
            started = True

    for bi in range(4):
        if bi >= 2:
            pltpu.make_async_copy(obuf.at[bi % 2], lower_ref.at[pl.ds((bi - 2) * BLOCK, BLOCK)], out_sem.at[2 + bi % 2]).wait()
        for kb in range(4):
            for h in range(2):
                cols = pl.ds((2 * kb + h) * BLOCK, BLOCK)
                if kb <= bi:
                    obuf[bi % 2, :, cols] = acc[h, bi, :, kb * BLOCK:(kb + 1) * BLOCK].astype(jnp.bfloat16)
                else:
                    obuf[bi % 2, :, cols] = jnp.zeros((BLOCK, BLOCK), jnp.bfloat16)
        pltpu.make_async_copy(obuf.at[bi % 2], lower_ref.at[pl.ds(bi * BLOCK, BLOCK)], out_sem.at[2 + bi % 2]).start()
    for kb in range(4):
        for i in range(2):
            arrive(got.at[kb, i], got_recv.at[kb, i])
        rbuf[kb * BLOCK:(kb + 1) * BLOCK] = (part[kb, 2] + got[kb, 0] + got[kb, 1]).astype(jnp.bfloat16)
    out = pltpu.make_async_copy(rbuf, right_ref, out_sem.at[4])
    out.start()

    def sent(ref, i):
        pltpu.make_async_copy(ref, ref, send_sem.at[i]).wait()

    def pieces(n):
        return low_all.at[pl.ds(0, n // 4)] if n >= 4 else low_all.at[0, pl.ds(0, n)]

    @pl.when(jnp.logical_not(side_self))
    def _():
        sent(side_all.at[0], 0)

    @pl.when(hub)
    def _():
        sent(pieces(1), 1)
        sent(pieces(8), 5)

    @pl.when(jnp.logical_not(hub))
    def _():
        sent(pieces(2), 1)
        sent(pieces(4), 5)

    sent(side_all.at[pl.ds(0, 15)], 2)
    sent(grad_all.at[pl.ds(0, 3)], 3)
    sent(line_all.at[pl.ds(0, 7)], 4)
    sent(pieces(8), 6)
    sent(part.at[:, 0], 7)
    sent(got, 8)
    for bi in (2, 3):
        pltpu.make_async_copy(obuf.at[bi % 2], lower_ref.at[pl.ds(bi * BLOCK, BLOCK)], out_sem.at[2 + bi % 2]).wait()
    out.wait()


def fused(low, side, grad):
    dt = low.dtype
    f32 = jnp.float32
    anywhere = pl.BlockSpec(memory_space=pl.ANY)
    dma = pltpu.SemaphoreType.DMA
    return pl.pallas_call(
        kernel,
        out_shape=[jax.ShapeDtypeStruct(grad.shape, dt), jax.ShapeDtypeStruct(low.shape, dt),
                   jax.ShapeDtypeStruct((4, 4, 2560, BLOCK), dt)],
        in_specs=[anywhere] * 3,
        out_specs=[anywhere] * 3,
        scratch_shapes=[
            pltpu.VMEM((16, 1024, 512), dt),
            pltpu.VMEM((4, 1024, 512), dt),
            pltpu.VMEM((8, 1024, 512), dt),
            pltpu.VMEM((2, 4, BLOCK, 1024), f32),
            pltpu.VMEM((4, 4, BLOCK, 512), f32),
            pltpu.VMEM((4, 2, 128, 512), f32),
            pltpu.VMEM((4, 2, BLOCK, 512), f32),
            pltpu.VMEM((2, 4, 1024, BLOCK), dt),
            pltpu.VMEM((2560, BLOCK), dt),
            pltpu.VMEM((2, BLOCK, 2048), dt),
            pltpu.VMEM((1024, 512), dt),
            dma((4, 4, 4)), dma((16, 4)), dma((4, 2)), dma((8, 2)), dma((4, 2)), dma((4, 2)),
            dma((9,)), dma((2,)), dma((4,)), dma((5,)),
        ],
        compiler_params=pltpu.CompilerParams(has_side_effects=True, vmem_limit_bytes=67043328),
        name="fused",
    )(low, side.reshape(4, BLOCK, 512), grad)


def per_device(low, side, grad):
    right, lower, _ = fused(low, side, grad)
    row_pos = jnp.arange(lower.shape[0])[:, None]
    col_pos = jnp.arange(lower.shape[1])[None, :]
    row_global = (row_pos // BLOCK * 16 + lax.axis_index("row")) * BLOCK + row_pos % BLOCK
    col_global = (col_pos // BLOCK * 8 + lax.axis_index("col")) * BLOCK + col_pos % BLOCK
    return right, jnp.where(row_global >= col_global, lower, jnp.zeros_like(lower))


def solution(mesh):
    spec = P(("batch", "row"), "col")
    return jax.shard_map(per_device, mesh=mesh, in_specs=(spec,) * 3, out_specs=(spec,) * 2, check_vma=False)
```

```python
import jax
import jax.numpy as jnp
from jax import lax
from jax.experimental import pallas as pl
from jax.experimental.pallas import tpu as pltpu
from jax.sharding import PartitionSpec as P

BLOCK = 256
MESH = pl.DeviceIdType.MESH
NROWS = (1024, 768, 512, 256)
FIRST = (0, 1024, 1792, 2304)
LAG = 2.5


def plan():
    ready, jobs, steps = {}, [], []

    def job(need, link, cost, made, prio, step):
        jobs.append((need, link, cost, made, prio, step))

    for q in range(4):
        first = 1 if q < 2 else 0
        def hop(off, axis, d):
            moved = list(off)
            moved[axis] = (moved[axis] - d) % 4
            return tuple(moved)
        ready[("mid", q)] = 8.0 + 6.0 * q
        job(("mid", q), "spread", 6.0, ("side", (0, 0), q), 0, ("spread", q))
        for lane in (None, 0, 1, 3, 2):
            axis = first if lane is None else 1 - first
            own = [0, 0]
            if lane is not None:
                own[first] = lane
            own = tuple(own)
            prio = 1 if lane is None else 5
            for d in (1, -1):
                job(("side", own, q), ("zy"[axis], d), 5.65, ("side", hop(own, axis, d), q), prio, ("side", own, q, axis, d))
            d = 1 if q % 2 == 0 else -1
            near = hop(own, axis, d)
            job(("side", near, q), ("zy"[axis], d), 5.65, ("side", hop(near, axis, d), q), prio, ("side", near, q, axis, d))
    for half in range(2):
        ready[("grad", 0, half)] = 0.0
        ready[("line", "own", half)] = 0.0
        for d in (1, -1):
            job(("grad", 0, half), ("z", d), 11.3, ("grad", -d % 4, half), 3, ("grad", 0, half, d))
        d = 1 if half == 0 else -1
        job(("grad", -d % 4, half), ("z", d), 11.3, ("grad", 2, half), 3, ("grad", -d % 4, half, d))
        for to in "ab":
            job(("line", "own", half), to, 11.3, ("line", to, half), 4, ("line", "own", half, to))
        src, to = ("a", "b") if half == 0 else ("b", "a")
        job(("line", src, half), to, 11.3, ("line", "o", half), 4, ("line", src, half, to))
        for piece in ("own", "a", "b", "o"):
            job(("line", piece, half), "sib", 1.0, ("line", piece + "s", half), 4, ("line", piece, half, "sib"))
    ready[("move", 0)] = 0.0
    for kb in range(4):
        cost = 11.3 * NROWS[kb] / 1024
        for d in (1, -1):
            job(("move", kb), ("z", d), 1.5 * cost, ("move", kb + 1) if d == 1 else ("moved", kb), (0, 0, 4, 4)[kb], ("move", kb, d))
        for zz in range(4):
            job(("hub", kb, zz), "b", cost, ("p", kb, zz), 2 + 0.1 * kb, ("hub", kb, zz))
            job(("p", kb, zz), "a", cost, ("q", kb, zz), 2 + 0.1 * kb, ("p", kb, zz))
            job(("q", kb, zz), "sib", 0.1 * cost, ("qs", kb, zz), 2, ("q", kb, zz))
        ready[("hub", kb, 0)] = 4.0 + kb
    free = {}
    pending = list(jobs)
    while pending:
        best = min((j for j in pending if j[0] in ready),
                   key=lambda j: (max(ready[j[0]], free.get(j[1], 0.0)), j[4], ready[j[0]]))
        pending.remove(best)
        need, link, cost, made, prio, step = best
        start = max(ready[need], free.get(link, 0.0))
        free[link] = start + cost
        ready[made] = start + cost + LAG
        if made[0] == "move":
            ready[made] = start + cost
            for zz, extra in ((1, 0.0), (3, 0.0), (2, cost / 3)):
                ready[("hub", step[1], zz)] = start + cost + LAG + extra
        steps.append((max(ready[need], start - 12.0), start, ("send",) + step))
        for kb in range(4):
            key = ("sum", kb)
            if key not in ready and all(("qs", kb, zz) in ready for zz in range(4)) and ("grad", 2, 0) in ready and ("grad", 2, 1) in ready:
                now = max(t for e, t in ready.items() if e[:2] == ("qs", kb) or e[0] == "grad") + 3.0
                ready[key] = now
                steps.append((now, now, ("part", kb)))
                for d in (1, -1):
                    pending.append((key, ("y", d), 5.65, ("hop", kb, d), 0, ("far", kb, d)))
                    pending.append((("hop", kb, d), ("y", d), 11.3, ("got", kb, d), 0, ("near", kb, d)))
    slots = sorted((max(ready[("side", (a, b), q)] for q in range(4)), (a, b)) for a in range(4) for b in range(4))
    for g in range(4):
        steps.append((1e4 + (g // 2) * 10, g, ("dot", tuple(off for _, off in slots[4 * g:4 * g + 4]))))
    steps = [(1e4 + 5, b, s) if s[:3] == ("send", "near", 3) else (a, b, s) for a, b, s in steps]
    steps.sort(key=lambda t: (t[0], t[1]))
    return [s for _, _, s in steps], ready


def kernel(low_ref, side_ref, grad_ref, right_ref, lower_ref, low_all,
           side_all, grad_all, line_all, acc, part, hop, got, lbuf, stage, obuf, rbuf,
           mid, low_recv, side_recv, grad_recv, line_recv, hop_recv, got_recv, mid_recv, send_sem, lbuf_sem, stage_sem, out_sem):
    r, c = lax.axis_index("row"), lax.axis_index("col")
    z, y, x, core = r // 4, r % 4, c // 2, c % 2
    hub = x // 2 == z % 2
    xa, xb = x + 1 - 2 * (x % 2), 3 - x
    xh = jnp.where(hub, x, xb)

    def bxor(a, b):
        return sum(((a // n % 2 + b // n % 2) % 2) * n for n in (1, 2, 4))

    def place(zz, yy, xx, cc):
        return {"row": zz * 4 + yy, "col": xx * 2 + cc}

    def remote(src, dst, send, recv, to):
        return pltpu.make_async_remote_copy(src, dst, send_sem.at[send], recv, device_id=to, device_id_type=MESH)

    def arrive(ref, sem):
        pltpu.make_async_copy(ref, ref, sem).wait()

    sib = place(z, y, x, 1 - core)
    up, down = place(z, (y + 1) % 4, x, core), place(z, (y + 3) % 4, x, core)

    turn = bxor(c, r % 8)
    side_row = (r // 8) * 8 + turn

    def quarter(ref, q):
        return ref.at[pl.ds(q * BLOCK, BLOCK)]

    @pl.when((c != 0) & (turn != 0))
    def _():
        for q in range(4):
            remote(quarter(side_ref, q), quarter(mid, q), 0, mid_recv.at[q], {"row": side_row, "col": c}).start()

    @pl.when((c != 0) & (turn == 0))
    def _():
        for q in range(4):
            remote(quarter(side_ref, q), quarter(side_all.at[side_row], q), 0, side_recv.at[side_row, q],
                   {"row": side_row, "col": c}).start()

    @pl.when((c == 0) & (turn == 0))
    def _():
        for q in range(4):
            pltpu.make_async_copy(quarter(side_ref, q), quarter(side_all.at[r], q), side_recv.at[r, q]).start()

    def spread(q):
        to = {"row": r, "col": turn}

        @pl.when((r % 8 != 0) & (c != 0))
        def _():
            arrive(quarter(mid, q), mid_recv.at[q])
            remote(quarter(mid, q), quarter(side_all.at[r], q), 9, side_recv.at[r, q], to).start()

        @pl.when((r % 8 != 0) & (c == 0))
        def _():
            remote(quarter(side_ref, q), quarter(side_all.at[r], q), 9, side_recv.at[r, q], to).start()

    mine = 2 * (x % 2) + core

    def low_piece(h, kb):
        return low_ref.at[pl.ds(kb * BLOCK, NROWS[kb]), pl.ds(pl.multiple_of((2 * kb + h) * BLOCK, BLOCK), BLOCK)]

    def low_at(yy, zz, kb):
        return low_all.at[yy, zz, pl.ds(FIRST[kb], NROWS[kb])]

    def stage_at(kb):
        return stage.at[pl.ds(FIRST[kb], NROWS[kb])]

    here = z // 2

    @pl.when(hub)
    def _():
        for kb in range(4):
            pltpu.make_async_copy(low_piece(here, kb), stage_at(kb), stage_sem.at[kb]).start()

    def move(kb):
        @pl.when(hub)
        def _():
            remote(low_piece(1 - here, kb), low_at(mine, z, kb), 1, low_recv.at[mine, z, kb],
                   place((z + 2) % 4, y, x, core)).start()

        @pl.when(jnp.logical_not(hub))
        def _():
            for h in range(2):
                remote(low_piece(h, kb), low_at(mine, z, kb), 1, low_recv.at[mine, z, kb],
                       place(x // 2 + 2 * h, y, x, core)).start()

    move(0)

    own_grad = pltpu.make_async_copy(grad_ref, grad_all.at[z], out_sem.at[0])
    own_line = pltpu.make_async_copy(grad_ref, line_all.at[c], out_sem.at[1])
    own_grad.start()
    own_line.start()

    @pl.when(hub)
    def _():
        for kb in range(4):
            pltpu.make_async_copy(low_piece(here, kb), stage_at(kb), stage_sem.at[kb]).wait()
            pltpu.make_async_copy(stage_at(kb), low_at(mine, z, kb), low_recv.at[mine, z, kb]).start()

    steps, ready = plan()
    waited = set()

    def line_slot(piece):
        xx = {"own": x, "a": xa, "b": xb, "o": (x + 2) % 4}[piece.rstrip("s")]
        return xx * 2 + (1 - core if piece.endswith("s") else core)

    def half_at(ref, slot, half):
        return ref.at[slot, pl.ds(half * 512, 512)]

    def wait(event):
        if event in waited:
            return
        waited.add(event)
        name = event[0]
        if name == "side":
            slot = ((z + event[1][0]) % 4) * 4 + (y + event[1][1]) % 4
            arrive(side_all.at[slot, pl.ds(event[2] * BLOCK, BLOCK)], side_recv.at[slot, event[2]])
        elif name == "grad":
            slot = (z + event[1]) % 4
            arrive(half_at(grad_all, slot, event[2]), grad_recv.at[slot, event[2]])
        elif name == "line":
            slot = line_slot(event[1])
            arrive(half_at(line_all, slot, event[2]), line_recv.at[slot, event[2]])
        else:
            yy = 2 * (xh % 2 if name in ("p", "ps") else 1 - xh % 2) + (1 - core if name.endswith("s") else core)
            zz = (z + event[2]) % 4
            arrive(low_at(yy, zz, event[1]), low_recv.at[yy, zz, event[1]])

    def low_send(yy, zz, kb, send, to):
        remote(low_at(yy, zz, kb), low_at(yy, zz, kb), send, low_recv.at[yy, zz, kb], to).start()

    def send(step):
        name = step[0]
        if name == "spread":
            spread(step[1])
        elif name == "move":
            if step[1] and step[2] == 1:
                move(step[1])
        elif name == "side":
            _, off, q, axis, d = step
            wait(("side", off, q))
            slot = ((z + off[0]) % 4) * 4 + (y + off[1]) % 4
            to = place((z + d + 4) % 4, y, x, core) if axis == 0 else place(z, (y + d + 4) % 4, x, core)
            ref = side_all.at[slot, pl.ds(q * BLOCK, BLOCK)]
            remote(ref, ref, 2, side_recv.at[slot, q], to).start()
        elif name == "grad":
            _, off, half, d = step
            if off:
                wait(("grad", off, half))
            slot = (z + off) % 4
            src = half_at(grad_all, slot, half) if off else grad_ref.at[pl.ds(half * 512, 512)]
            remote(src, half_at(grad_all, slot, half), 3, grad_recv.at[slot, half], place((z + d + 4) % 4, y, x, core)).start()
        elif name == "line":
            _, piece, half, to = step
            if piece != "own":
                wait(("line", piece, half))
            slot = line_slot(piece)
            src = half_at(line_all, slot, half) if piece != "own" else grad_ref.at[pl.ds(half * 512, 512)]
            dest = {"a": place(z, y, xa, core), "b": place(z, y, xb, core), "sib": sib}[to]
            remote(src, half_at(line_all, slot, half), 4, line_recv.at[slot, half], dest).start()
        elif name == "hub":
            _, kb, dz = step
            zz = (z + dz) % 4

            @pl.when(hub)
            def _():
                yy = mine
                arrive(low_at(yy, zz, kb), low_recv.at[yy, zz, kb])
                low_send(yy, zz, kb, 5, place(z, y, xb, core))
                low_send(yy, zz, kb, 5, place(z, y, xa, core))
                low_send(yy, zz, kb, 6, sib)
        elif name == "p":
            _, kb, dz = step
            zz = (z + dz) % 4
            yy = 2 * (xb % 2) + core

            @pl.when(jnp.logical_not(hub))
            def _():
                arrive(low_at(yy, zz, kb), low_recv.at[yy, zz, kb])
                low_send(yy, zz, kb, 5, place(z, y, xa, core))
                low_send(yy, zz, kb, 6, sib)
        elif name == "q":
            _, kb, dz = step
            zz = (z + dz) % 4
            wait(("q", kb, dz))
            low_send(2 * (1 - xh % 2) + core, zz, kb, 6, sib)
        elif name == "far":
            _, kb, d = step
            i = 0 if d == 1 else 1
            rows = pl.ds(i * 128, 128)
            remote(part.at[kb, 0, rows], hop.at[kb, i], 7, hop_recv.at[kb, i], up if d == 1 else down).start()
        elif name == "near":
            _, kb, d = step
            i, t = (0, 3) if d == 1 else (1, 1)
            arrive(hop.at[kb, i], hop_recv.at[kb, i])
            rows = pl.ds(i * 128, 128)
            part[kb, t, rows] += hop[kb, i]
            remote(part.at[kb, t], got.at[kb, i], 8, got_recv.at[kb, i], up if d == 1 else down).start()

    def add_part(kb):
        for zz in range(4):
            for name in ("ps", "q", "qs"):
                wait((name, kb, zz))
        if kb == 0:
            own_grad.wait()
            for off in (1, 2, 3):
                for half in range(2):
                    wait(("grad", off, half))
        n = NROWS[kb]

        def load(t):
            return pltpu.make_async_copy(low_all.at[(y + 2 + t) % 4, :, pl.ds(FIRST[kb], n)],
                                         lbuf.at[t % 2, :, pl.ds(0, n)], lbuf_sem.at[t % 2])

        load(0).start()

        def body(t, carry):
            @pl.when(t < 3)
            def _():
                load(t + 1).start()
            load(t).wait()
            total = jnp.zeros((BLOCK, 512), jnp.float32)
            for zz in range(4):
                total += lax.dot_general(lbuf[t % 2, zz, pl.ds(0, n)], grad_all[zz, pl.ds(kb * BLOCK, n)],
                                         (((0,), (0,)), ((), ())), preferred_element_type=jnp.float32)
            part[kb, t] = total
            return carry

        lax.fori_loop(0, 4, body, 0)

    def add_dot(offs, start):
        if start:
            own_line.wait()
            for piece in ("a", "b", "o", "owns", "as", "bs", "os"):
                for half in range(2):
                    wait(("line", piece, half))
            acc[...] = jnp.zeros_like(acc)
        slots = []
        for off in offs:
            for q in range(4):
                wait(("side", off, q))
            slots.append(((z + off[0]) % 4) * 4 + (y + off[1]) % 4)

        def body(i, carry):
            slot = slots[3]
            for n in range(3):
                slot = jnp.where(i == n, slots[n], slot)
            h, cj = slot // 8, bxor(slot % 8, c)
            for bi in range(4):
                n = (bi + 1) * BLOCK
                acc[h, bi, :, :n] += lax.dot_general(
                    line_all[cj, bi * BLOCK:(bi + 1) * BLOCK], side_all[slot, :n],
                    (((1,), (1,)), ((), ())), preferred_element_type=jnp.float32)
            return carry

        lax.fori_loop(0, 4, body, 0)

    started = False
    for step in steps:
        if step[0] == "send":
            send(step[1:])
        elif step[0] == "part":
            add_part(step[1])
        else:
            add_dot(step[1], not started)
            started = True

    for bi in range(4):
        if bi >= 2:
            pltpu.make_async_copy(obuf.at[bi % 2], lower_ref.at[pl.ds((bi - 2) * BLOCK, BLOCK)], out_sem.at[2 + bi % 2]).wait()
        for kb in range(4):
            for h in range(2):
                cols = pl.ds((2 * kb + h) * BLOCK, BLOCK)
                if kb <= bi:
                    obuf[bi % 2, :, cols] = acc[h, bi, :, kb * BLOCK:(kb + 1) * BLOCK].astype(jnp.bfloat16)
                else:
                    obuf[bi % 2, :, cols] = jnp.zeros((BLOCK, BLOCK), jnp.bfloat16)
        pltpu.make_async_copy(obuf.at[bi % 2], lower_ref.at[pl.ds(bi * BLOCK, BLOCK)], out_sem.at[2 + bi % 2]).start()
    for kb in range(4):
        for i in range(2):
            arrive(got.at[kb, i], got_recv.at[kb, i])
        rbuf[kb * BLOCK:(kb + 1) * BLOCK] = (part[kb, 2] + got[kb, 0] + got[kb, 1]).astype(jnp.bfloat16)
    out = pltpu.make_async_copy(rbuf, right_ref, out_sem.at[4])
    out.start()

    def sent(ref, i):
        pltpu.make_async_copy(ref, ref, send_sem.at[i]).wait()

    def pieces(n):
        return low_all.at[pl.ds(0, n // 4)] if n >= 4 else low_all.at[0, pl.ds(0, n)]

    @pl.when(c != 0)
    def _():
        sent(side_all.at[0], 0)

    @pl.when(r % 8 != 0)
    def _():
        sent(side_all.at[0], 9)

    @pl.when(hub)
    def _():
        sent(pieces(1), 1)
        sent(pieces(8), 5)

    @pl.when(jnp.logical_not(hub))
    def _():
        sent(pieces(2), 1)
        sent(pieces(4), 5)

    sent(side_all.at[pl.ds(0, 15)], 2)
    sent(grad_all.at[pl.ds(0, 3)], 3)
    sent(line_all.at[pl.ds(0, 7)], 4)
    sent(pieces(8), 6)
    sent(part.at[:, 0], 7)
    sent(got, 8)
    for bi in (2, 3):
        pltpu.make_async_copy(obuf.at[bi % 2], lower_ref.at[pl.ds(bi * BLOCK, BLOCK)], out_sem.at[2 + bi % 2]).wait()
    out.wait()


def fused(low, side, grad):
    dt = low.dtype
    f32 = jnp.float32
    anywhere = pl.BlockSpec(memory_space=pl.ANY)
    dma = pltpu.SemaphoreType.DMA
    return pl.pallas_call(
        kernel,
        out_shape=[jax.ShapeDtypeStruct(grad.shape, dt), jax.ShapeDtypeStruct(low.shape, dt),
                   jax.ShapeDtypeStruct((4, 4, 2560, BLOCK), dt)],
        in_specs=[anywhere] * 3,
        out_specs=[anywhere] * 3,
        scratch_shapes=[
            pltpu.VMEM((16, 1024, 512), dt),
            pltpu.VMEM((4, 1024, 512), dt),
            pltpu.VMEM((8, 1024, 512), dt),
            pltpu.VMEM((2, 4, BLOCK, 1024), f32),
            pltpu.VMEM((4, 4, BLOCK, 512), f32),
            pltpu.VMEM((4, 2, 128, 512), f32),
            pltpu.VMEM((4, 2, BLOCK, 512), f32),
            pltpu.VMEM((2, 4, 1024, BLOCK), dt),
            pltpu.VMEM((2560, BLOCK), dt),
            pltpu.VMEM((2, BLOCK, 2048), dt),
            pltpu.VMEM((1024, 512), dt),
            pltpu.VMEM((1024, 512), dt),
            dma((4, 4, 4)), dma((16, 4)), dma((4, 2)), dma((8, 2)), dma((4, 2)), dma((4, 2)), dma((4,)),
            dma((10,)), dma((2,)), dma((4,)), dma((5,)),
        ],
        compiler_params=pltpu.CompilerParams(has_side_effects=True, vmem_limit_bytes=67043328),
        name="fused",
    )(low, side, grad)


def per_device(low, side, grad):
    right, lower, _ = fused(low, side, grad)
    row_pos = jnp.arange(lower.shape[0])[:, None]
    col_pos = jnp.arange(lower.shape[1])[None, :]
    row_global = (row_pos // BLOCK * 16 + lax.axis_index("row")) * BLOCK + row_pos % BLOCK
    col_global = (col_pos // BLOCK * 8 + lax.axis_index("col")) * BLOCK + col_pos % BLOCK
    return right, jnp.where(row_global >= col_global, lower, jnp.zeros_like(lower))


def solution(mesh):
    spec = P(("batch", "row"), "col")
    return jax.shard_map(per_device, mesh=mesh, in_specs=(spec,) * 3, out_specs=(spec,) * 2, check_vma=False)
```

```python
import jax
import jax.numpy as jnp
from jax import lax
from jax.experimental import pallas as pl
from jax.experimental.pallas import tpu as pltpu
from jax.sharding import PartitionSpec as P

BLOCK = 256
MESH = pl.DeviceIdType.MESH
NROWS = (1024, 768, 512, 256)
FIRST = (0, 1024, 1792, 2304)
ORDER = (3, 1, 0, 2)
LAG = 2.5


def plan():
    ready, jobs, steps = {}, [], []

    def job(need, link, cost, made, prio, step):
        jobs.append((need, link, cost, made, prio, step))

    for q in range(4):
        first = 1 if q < 2 else 0
        def hop(off, axis, d):
            moved = list(off)
            moved[axis] = (moved[axis] - d) % 4
            return tuple(moved)
        ready[("mid", q)] = 16.0 + 8.0 * q
        job(("mid", q), "spread", 8.0, ("side", (0, 0), q), 0, ("spread", q))
        job(("mid", q), "a", 5.65, ("spread a", q), 0, ("none",))
        job(("mid", q), "b", 5.65, ("spread b", q), 0, ("none",))
        for lane in (None, 0, 1, 3, 2):
            axis = first if lane is None else 1 - first
            own = [0, 0]
            if lane is not None:
                own[first] = lane
            own = tuple(own)
            prio = 1 if lane is None else 5
            for d in (1, -1):
                job(("side", own, q), ("zy"[axis], d), 5.65, ("side", hop(own, axis, d), q), prio, ("side", own, q, axis, d))
            d = 1 if q % 2 == 0 else -1
            near = hop(own, axis, d)
            job(("side", near, q), ("zy"[axis], d), 5.65, ("side", hop(near, axis, d), q), prio, ("side", near, q, axis, d))
    for half in (1, 0):
        ready[("grad", 0, half)] = 0.0
        ready[("line", "own", half)] = 110.0 * (1 - half)
        for d in (1, -1):
            job(("grad", 0, half), ("z", d), 11.3, ("grad", -d % 4, half), 2 - half, ("grad", 0, half, d))
        d = 1 if half == 0 else -1
        job(("grad", -d % 4, half), ("z", d), 11.3, ("grad", 2, half), 2 - half, ("grad", -d % 4, half, d))
        for to in "ab":
            job(("line", "own", half), to, 11.3, ("line", to, half), 4, ("line", "own", half, to))
        src, to = ("a", "b") if half == 0 else ("b", "a")
        job(("line", src, half), to, 11.3, ("line", "o", half), 4, ("line", src, half, to))
        for piece in ("own", "a", "b", "o"):
            job(("line", piece, half), "sib", 1.0, ("line", piece + "s", half), 4, ("line", piece, half, "sib"))
    ready[("move", ORDER[0])] = 0.0
    ready[("hub", "end", 0)] = 0.0
    for n, kb in enumerate(ORDER):
        cost = 11.3 * NROWS[kb] / 1024
        for d in (1, -1):
            job(("move", kb), ("z", d), 1.5 * cost, ("move", (ORDER + ("end",))[n + 1]) if d == 1 else ("moved", kb), (0, 0, 0.5, 1.5)[n], ("move", kb, d))
        for zz in range(4):
            job(("hub", kb, zz), "b", cost, ("p", kb, zz), 2 + 0.1 * n, ("hub", kb, zz))
            job(("p", kb, zz), "a", cost, ("q", kb, zz), 2 + 0.1 * n, ("p", kb, zz))
            job(("q", kb, zz), "sib", 0.1 * cost, ("qs", kb, zz), 2, ("q", kb, zz))
        ready[("hub", kb, 0)] = 4.0 + n
    free = {}
    pending = list(jobs)
    while pending:
        best = min((j for j in pending if j[0] in ready),
                   key=lambda j: (max(ready[j[0]], free.get(j[1], 0.0)), j[4], ready[j[0]]))
        pending.remove(best)
        need, link, cost, made, prio, step = best
        start = max(ready[need], free.get(link, 0.0))
        free[link] = start + cost
        ready[made] = start + cost + LAG
        if made[0] == "move":
            ready[made] = start + cost
            for zz, extra in ((1, 0.0), (3, 0.0), (2, cost / 3)):
                ready[("hub", step[1], zz)] = start + cost + LAG + extra
        steps.append((max(ready[need], start - 12.0), start, ("send",) + step))
        for kb in ORDER:
            key = ("sum", kb)
            if key not in ready and all(("qs", kb, zz) in ready for zz in range(4)) and ("grad", 2, 1) in ready and (kb > 1 or ("grad", 2, 0) in ready):
                now = max(t for e, t in ready.items() if e[:2] == ("qs", kb) or e[0] == "grad" and (kb < 2 or e[2] == 1)) + 3.0
                ready[key] = now
                steps.append((now, now, ("part", kb)))
                for d in (1, -1):
                    pending.append((key, ("y", d), 5.65, ("hop", kb, d), 0, ("none",)))
                    pending.append((("hop", kb, d), ("y", d), 11.3, ("got", kb, d), 0, ("near", kb, d)))
    for g in range(4):
        steps.append((1e4 + (g // 2) * 10, g, ("dot", ("own", "a", "b", "o")[g])))
    steps = [(1e4 + 5, b, s) if s[:3] == ("send", "near", ORDER[-1]) else (a, b, s) for a, b, s in steps]
    steps.sort(key=lambda t: (t[0], t[1]))
    return [s for _, _, s in steps], ready


def kernel(low_ref, side_ref, grad_ref, right_ref, lower_ref, low_all,
           side_all, grad_all, line_all, acc, part, hop, got, lbuf, stage, obuf, rbuf,
           mid, low_recv, side_recv, grad_recv, line_recv, hop_recv, got_recv, mid_recv, send_sem, lbuf_sem, stage_sem, out_sem):
    r, c = lax.axis_index("row"), lax.axis_index("col")
    z, y, x, core = r // 4, r % 4, c // 2, c % 2
    hub = x // 2 == z % 2
    xa, xb = x + 1 - 2 * (x % 2), 3 - x
    xh = jnp.where(hub, x, xb)

    def place(zz, yy, xx, cc):
        return {"row": zz * 4 + yy, "col": xx * 2 + cc}

    def remote(src, dst, send, recv, to):
        return pltpu.make_async_remote_copy(src, dst, send_sem.at[send], recv, device_id=to, device_id_type=MESH)

    def arrive(ref, sem):
        pltpu.make_async_copy(ref, ref, sem).wait()

    sib = place(z, y, x, 1 - core)
    up, down = place(z, (y + 1) % 4, x, core), place(z, (y + 3) % 4, x, core)

    def shift(sig, kk):
        return (sig + kk * (5 - 2 * sig)) % 4

    def spread_row(cj, cc):
        return 2 * shift((cc // 2 + 4 - cj // 2) % 4, cj % 2) + (cj + cc) % 2

    def spread_col(row8, cj):
        return 2 * ((cj // 2 + shift(row8 // 2, cj % 2)) % 4) + (cj + row8) % 2

    def spread_from(row8, cc):
        kk = (cc + row8) % 2
        return 2 * ((cc // 2 + 4 - shift(row8 // 2, kk)) % 4) + kk

    side_row = (r // 8) * 8 + spread_row(c, r % 8)
    side_col = spread_col(r % 8, c)
    stays, direct = side_row == r, c == r % 8

    def quarter(ref, q):
        return ref.at[pl.ds(q * BLOCK, BLOCK)]

    def spread_first():
        @pl.when(jnp.logical_not(stays) & jnp.logical_not(direct))
        def _():
            for q in range(4):
                remote(quarter(side_ref, q), quarter(mid, q), 0, mid_recv.at[q], {"row": side_row, "col": c}).start()

        @pl.when(jnp.logical_not(stays) & direct)
        def _():
            for q in range(4):
                remote(quarter(side_ref, q), quarter(side_all.at[side_row], q), 0, side_recv.at[side_row, q],
                       {"row": side_row, "col": c}).start()

        @pl.when(stays & direct)
        def _():
            for q in range(4):
                pltpu.make_async_copy(quarter(side_ref, q), quarter(side_all.at[r], q), side_recv.at[r, q]).start()

    def spread(q):
        to = {"row": r, "col": side_col}

        @pl.when((side_col != c) & (side_col != r % 8))
        def _():
            arrive(quarter(mid, q), mid_recv.at[q])
            remote(quarter(mid, q), quarter(side_all.at[r], q), 9, side_recv.at[r, q], to).start()

        @pl.when((side_col != c) & (side_col == r % 8))
        def _():
            remote(quarter(side_ref, q), quarter(side_all.at[r], q), 9, side_recv.at[r, q], to).start()

    mine = 2 * (x % 2) + core

    def low_piece(h, kb):
        return low_ref.at[pl.ds(kb * BLOCK, NROWS[kb]), pl.ds(pl.multiple_of((2 * kb + h) * BLOCK, BLOCK), BLOCK)]

    def low_at(yy, zz, kb):
        return low_all.at[yy, zz, pl.ds(FIRST[kb], NROWS[kb])]

    def stage_at(kb):
        return stage.at[pl.ds(FIRST[kb], NROWS[kb])]

    here = z // 2

    @pl.when(hub)
    def _():
        for kb in ORDER:
            pltpu.make_async_copy(low_piece(here, kb), stage_at(kb), stage_sem.at[kb]).start()

    def move(kb):
        @pl.when(hub)
        def _():
            remote(low_piece(1 - here, kb), low_at(mine, z, kb), 1, low_recv.at[mine, z, kb],
                   place((z + 2) % 4, y, x, core)).start()

        @pl.when(jnp.logical_not(hub))
        def _():
            for h in range(2):
                remote(low_piece(h, kb), low_at(mine, z, kb), 1, low_recv.at[mine, z, kb],
                       place(x // 2 + 2 * h, y, x, core)).start()

    move(ORDER[0])
    move(ORDER[1])
    spread_first()

    own_grad = pltpu.make_async_copy(grad_ref, grad_all.at[z], out_sem.at[0])
    own_line = pltpu.make_async_copy(grad_ref, line_all.at[c], out_sem.at[1])
    own_grad.start()
    own_line.start()

    @pl.when(hub)
    def _():
        for kb in ORDER:
            pltpu.make_async_copy(low_piece(here, kb), stage_at(kb), stage_sem.at[kb]).wait()
            pltpu.make_async_copy(stage_at(kb), low_at(mine, z, kb), low_recv.at[mine, z, kb]).start()

    steps, ready = plan()
    waited = set()

    def line_slot(piece):
        xx = {"own": x, "a": xa, "b": xb, "o": (x + 2) % 4}[piece.rstrip("s")]
        return xx * 2 + (1 - core if piece.endswith("s") else core)

    def half_at(ref, slot, half):
        return ref.at[slot, pl.ds(half * 512, 512)]

    def wait(event):
        if event in waited:
            return
        waited.add(event)
        name = event[0]
        if name == "side":
            slot = ((z + event[1][0]) % 4) * 4 + (y + event[1][1]) % 4
            arrive(side_all.at[slot, pl.ds(event[2] * BLOCK, BLOCK)], side_recv.at[slot, event[2]])
        elif name == "grad":
            slot = (z + event[1]) % 4
            arrive(half_at(grad_all, slot, event[2]), grad_recv.at[slot, event[2]])
        elif name == "line":
            slot = line_slot(event[1])
            arrive(half_at(line_all, slot, event[2]), line_recv.at[slot, event[2]])
        else:
            yy = 2 * (xh % 2 if name in ("p", "ps") else 1 - xh % 2) + (1 - core if name.endswith("s") else core)
            zz = (z + event[2]) % 4
            arrive(low_at(yy, zz, event[1]), low_recv.at[yy, zz, event[1]])

    def low_send(yy, zz, kb, send, to):
        remote(low_at(yy, zz, kb), low_at(yy, zz, kb), send, low_recv.at[yy, zz, kb], to).start()

    def send(step):
        name = step[0]
        if name == "spread":
            spread(step[1])
        elif name == "move":
            if step[1] in ORDER[2:] and step[2] == 1:
                move(step[1])
        elif name == "side":
            _, off, q, axis, d = step
            wait(("side", off, q))
            slot = ((z + off[0]) % 4) * 4 + (y + off[1]) % 4
            to = place((z + d + 4) % 4, y, x, core) if axis == 0 else place(z, (y + d + 4) % 4, x, core)
            ref = side_all.at[slot, pl.ds(q * BLOCK, BLOCK)]
            remote(ref, ref, 2, side_recv.at[slot, q], to).start()
        elif name == "grad":
            _, off, half, d = step
            if off:
                wait(("grad", off, half))
            slot = (z + off) % 4
            src = half_at(grad_all, slot, half) if off else grad_ref.at[pl.ds(half * 512, 512)]
            remote(src, half_at(grad_all, slot, half), 3, grad_recv.at[slot, half], place((z + d + 4) % 4, y, x, core)).start()
        elif name == "line":
            _, piece, half, to = step
            if piece != "own":
                wait(("line", piece, half))
            slot = line_slot(piece)
            src = half_at(line_all, slot, half) if piece != "own" else grad_ref.at[pl.ds(half * 512, 512)]
            dest = {"a": place(z, y, xa, core), "b": place(z, y, xb, core), "sib": sib}[to]
            remote(src, half_at(line_all, slot, half), 4, line_recv.at[slot, half], dest).start()
        elif name == "hub":
            _, kb, dz = step
            zz = (z + dz) % 4

            @pl.when(hub)
            def _():
                yy = mine
                arrive(low_at(yy, zz, kb), low_recv.at[yy, zz, kb])
                low_send(yy, zz, kb, 5, place(z, y, xb, core))
                low_send(yy, zz, kb, 5, place(z, y, xa, core))
                low_send(yy, zz, kb, 6, sib)
        elif name == "p":
            _, kb, dz = step
            zz = (z + dz) % 4
            yy = 2 * (xb % 2) + core

            @pl.when(jnp.logical_not(hub))
            def _():
                arrive(low_at(yy, zz, kb), low_recv.at[yy, zz, kb])
                low_send(yy, zz, kb, 5, place(z, y, xa, core))
                low_send(yy, zz, kb, 6, sib)
        elif name == "q":
            _, kb, dz = step
            zz = (z + dz) % 4
            wait(("q", kb, dz))
            low_send(2 * (1 - xh % 2) + core, zz, kb, 6, sib)
        elif name == "far":
            _, kb, d = step
            i = 0 if d == 1 else 1
            rows = pl.ds(i * 128, 128)
            remote(part.at[kb, 0, rows], hop.at[kb, i], 7, hop_recv.at[kb, i], up if d == 1 else down).start()
        elif name == "near":
            _, kb, d = step
            i, t = (0, 3) if d == 1 else (1, 1)
            arrive(hop.at[kb, i], hop_recv.at[kb, i])
            rows = pl.ds(i * 128, 128)
            part[kb, t, rows] += hop[kb, i]
            remote(part.at[kb, t], got.at[kb, i], 8, got_recv.at[kb, i], up if d == 1 else down).start()

    def add_part(kb):
        for zz in range(4):
            for name in ("ps", "q", "qs"):
                wait((name, kb, zz))
        if kb == ORDER[0]:
            own_grad.wait()
        for off in (1, 2, 3):
            for half in (1,) if kb > 1 else (0, 1):
                wait(("grad", off, half))
        n = NROWS[kb]

        def load(t):
            return pltpu.make_async_copy(low_all.at[(y + 2 + t) % 4, :, pl.ds(FIRST[kb], n)],
                                         lbuf.at[t % 2, :, pl.ds(0, n)], lbuf_sem.at[t % 2])

        load(0).start()

        def body(t, carry):
            @pl.when(t < 3)
            def _():
                load(t + 1).start()
            load(t).wait()
            total = jnp.zeros((BLOCK, 512), jnp.float32)
            for zz in range(4):
                total += lax.dot_general(lbuf[t % 2, zz, pl.ds(0, n)], grad_all[zz, pl.ds(kb * BLOCK, n)],
                                         (((0,), (0,)), ((), ())), preferred_element_type=jnp.float32)
            part[kb, t] = total
            return carry

        body(0, 0)
        send(("far", kb, 1))
        send(("far", kb, -1))
        lax.fori_loop(1, 4, body, 0)

    def add_dot(piece, start):
        for name in (piece, piece + "s"):
            if name != "own":
                for half in range(2):
                    wait(("line", name, half))
        if start:
            own_line.wait()
            for a in range(4):
                for b in range(4):
                    for q in range(4):
                        wait(("side", (a, b), q))
        first = line_slot(piece) // 2

        def body(i, carry):
            cj = 2 * first + i % 2
            h = i // 2
            slot = 8 * h + spread_row(cj, c)
            for bi in range(4):
                n = (bi + 1) * BLOCK
                total = lax.dot_general(line_all[cj, bi * BLOCK:(bi + 1) * BLOCK], side_all[slot, :n],
                                        (((1,), (1,)), ((), ())), preferred_element_type=jnp.float32)
                acc[h, bi, :, :n] += total
            return carry

        if start:
            acc[...] = jnp.zeros_like(acc)
        lax.fori_loop(0, 4, body, 0)

    started = False
    for step in steps:
        if step[0] == "send":
            send(step[1:])
        elif step[0] == "part":
            add_part(step[1])
        else:
            add_dot(step[1], not started)
            started = True

    for bi in range(4):
        if bi >= 2:
            pltpu.make_async_copy(obuf.at[bi % 2], lower_ref.at[pl.ds((bi - 2) * BLOCK, BLOCK)], out_sem.at[2 + bi % 2]).wait()
        for kb in range(4):
            for h in range(2):
                cols = pl.ds((2 * kb + h) * BLOCK, BLOCK)
                if kb <= bi:
                    obuf[bi % 2, :, cols] = acc[h, bi, :, kb * BLOCK:(kb + 1) * BLOCK].astype(jnp.bfloat16)
                else:
                    obuf[bi % 2, :, cols] = jnp.zeros((BLOCK, BLOCK), jnp.bfloat16)
        pltpu.make_async_copy(obuf.at[bi % 2], lower_ref.at[pl.ds(bi * BLOCK, BLOCK)], out_sem.at[2 + bi % 2]).start()
    for kb in range(4):
        for i in range(2):
            arrive(got.at[kb, i], got_recv.at[kb, i])
        rbuf[kb * BLOCK:(kb + 1) * BLOCK] = (part[kb, 2] + got[kb, 0] + got[kb, 1]).astype(jnp.bfloat16)
    out = pltpu.make_async_copy(rbuf, right_ref, out_sem.at[4])
    out.start()

    def sent(ref, i):
        pltpu.make_async_copy(ref, ref, send_sem.at[i]).wait()

    def pieces(n):
        return low_all.at[pl.ds(0, n // 4)] if n >= 4 else low_all.at[0, pl.ds(0, n)]

    @pl.when(jnp.logical_not(stays))
    def _():
        sent(side_all.at[0], 0)

    @pl.when(side_col != c)
    def _():
        sent(side_all.at[0], 9)

    @pl.when(hub)
    def _():
        sent(pieces(1), 1)
        sent(pieces(8), 5)

    @pl.when(jnp.logical_not(hub))
    def _():
        sent(pieces(2), 1)
        sent(pieces(4), 5)

    sent(side_all.at[pl.ds(0, 15)], 2)
    sent(grad_all.at[pl.ds(0, 3)], 3)
    sent(line_all.at[pl.ds(0, 7)], 4)
    sent(pieces(8), 6)
    sent(part.at[:, 0], 7)
    sent(got, 8)
    for bi in (2, 3):
        pltpu.make_async_copy(obuf.at[bi % 2], lower_ref.at[pl.ds(bi * BLOCK, BLOCK)], out_sem.at[2 + bi % 2]).wait()
    out.wait()


def fused(low, side, grad):
    dt = low.dtype
    f32 = jnp.float32
    anywhere = pl.BlockSpec(memory_space=pl.ANY)
    dma = pltpu.SemaphoreType.DMA
    return pl.pallas_call(
        kernel,
        out_shape=[jax.ShapeDtypeStruct(grad.shape, dt), jax.ShapeDtypeStruct(low.shape, dt),
                   jax.ShapeDtypeStruct((4, 4, 2560, BLOCK), dt)],
        in_specs=[anywhere] * 3,
        out_specs=[anywhere] * 3,
        scratch_shapes=[
            pltpu.VMEM((16, 1024, 512), dt),
            pltpu.VMEM((4, 1024, 512), dt),
            pltpu.VMEM((8, 1024, 512), dt),
            pltpu.VMEM((2, 4, BLOCK, 1024), f32),
            pltpu.VMEM((4, 4, BLOCK, 512), f32),
            pltpu.VMEM((4, 2, 128, 512), f32),
            pltpu.VMEM((4, 2, BLOCK, 512), f32),
            pltpu.VMEM((2, 4, 1024, BLOCK), dt),
            pltpu.VMEM((2560, BLOCK), dt),
            pltpu.VMEM((2, BLOCK, 2048), dt),
            pltpu.VMEM((1024, 512), dt),
            pltpu.VMEM((1024, 512), dt),
            dma((4, 4, 4)), dma((16, 4)), dma((4, 2)), dma((8, 2)), dma((4, 2)), dma((4, 2)), dma((4,)),
            dma((10,)), dma((2,)), dma((4,)), dma((5,)),
        ],
        compiler_params=pltpu.CompilerParams(has_side_effects=True, vmem_limit_bytes=67043328),
        name="fused",
    )(low, side, grad)


def per_device(low, side, grad):
    right, lower, _ = fused(low, side, grad)
    row_pos = jnp.arange(lower.shape[0])[:, None]
    col_pos = jnp.arange(lower.shape[1])[None, :]
    row_global = (row_pos // BLOCK * 16 + lax.axis_index("row")) * BLOCK + row_pos % BLOCK
    col_global = (col_pos // BLOCK * 8 + lax.axis_index("col")) * BLOCK + col_pos % BLOCK
    return right, jnp.where(row_global >= col_global, lower, jnp.zeros_like(lower))


def solution(mesh):
    spec = P(("batch", "row"), "col")
    return jax.shard_map(per_device, mesh=mesh, in_specs=(spec,) * 3, out_specs=(spec,) * 2, check_vma=False)
```

```python
import jax
import jax.numpy as jnp
from jax import lax
from jax.experimental import pallas as pl
from jax.experimental.pallas import tpu as pltpu
from jax.sharding import PartitionSpec as P

BLOCK = 256
MESH = pl.DeviceIdType.MESH
NROWS = (1024, 768, 512, 256)
FIRST = (0, 1024, 1792, 2304)
ORDER = (3, 1, 0, 2)
SLACK = 5.0
LAG = 2.5


def plan():
    ready, jobs, steps = {}, [], []

    def job(need, link, cost, made, prio, step):
        jobs.append((need, link, cost, made, prio, step))

    for q in range(4):
        first = 1 if q < 2 else 0
        def hop(off, axis, d):
            moved = list(off)
            moved[axis] = (moved[axis] - d) % 4
            return tuple(moved)
        ready[("mid", q)] = 16.0 + 8.0 * q
        job(("mid", q), "spread", 8.0, ("side", (0, 0), q), 0, ("spread", q))
        job(("mid", q), "a", 2.8, ("spread a", q), 0, ("none",))
        job(("mid", q), "b", 2.8, ("spread b", q), 0, ("none",))
        for lane in (None, 0, 1, 3, 2):
            axis = first if lane is None else 1 - first
            own = [0, 0]
            if lane is not None:
                own[first] = lane
            own = tuple(own)
            prio = 1 if lane is None else 5
            for d in (1, -1):
                job(("side", own, q), ("zy"[axis], d), 5.65, ("side", hop(own, axis, d), q), prio, ("side", own, q, axis, d))
            d = 1 if q % 2 == 0 else -1
            near = hop(own, axis, d)
            job(("side", near, q), ("zy"[axis], d), 5.65, ("side", hop(near, axis, d), q), prio, ("side", near, q, axis, d))
    for half in (1, 0):
        ready[("grad", 0, half)] = 0.0
        ready[("line", "own", half)] = 0.0
        for d in (1, -1):
            job(("grad", 0, half), ("z", d), 11.3, ("grad", -d % 4, half), 2 - half, ("grad", 0, half, d))
        d = 1 if half == 0 else -1
        job(("grad", -d % 4, half), ("z", d), 11.3, ("grad", 2, half), 2 - half, ("grad", -d % 4, half, d))
        for to in "ab":
            job(("line", "own", half), to, 11.3, ("line", to, half), 1, ("line", "own", half, to))
        job(("late", "a", half), "b", 11.3, ("line", "o", half), 4, ("line", "a", half, "b"))
        ready[("late", "a", half)] = 130.0
        for piece in ("own", "a", "b", "o"):
            job(("line", piece, half), "sib", 1.0, ("line", piece + "s", half), 4, ("line", piece, half, "sib"))
    ready[("move", ORDER[0])] = 0.0
    ready[("hub", "end", 0)] = 0.0
    for n, kb in enumerate(ORDER):
        cost = 11.3 * NROWS[kb] / 1024
        for d in (1, -1):
            job(("move", kb), ("z", d), 1.5 * cost, ("move", (ORDER + ("end",))[n + 1]) if d == 1 else ("moved", kb), (0, 0, 0.5, 1.5)[n], ("move", kb, d))
        for zz in range(4):
            job(("hub", kb, zz), "b", cost, ("p", kb, zz), 2 + 0.1 * n, ("hub", kb, zz))
            job(("p", kb, zz), "a", cost, ("q", kb, zz), 2 + 0.1 * n, ("p", kb, zz))
            job(("q", kb, zz), "sib", 0.1 * cost, ("qs", kb, zz), 2, ("q", kb, zz))
        ready[("hub", kb, 0)] = 6.0 + 2 * n
        steps.append((2.0 + 2 * n, n, ("send", "stage", kb)))
    free = {}
    pending = list(jobs)
    while pending:
        best = min((j for j in pending if j[0] in ready),
                   key=lambda j: (max(ready[j[0]], free.get(j[1], 0.0)), j[4], ready[j[0]]))
        pending.remove(best)
        need, link, cost, made, prio, step = best
        start = max(ready[need], free.get(link, 0.0))
        free[link] = start + cost
        ready[made] = start + cost + LAG
        if made[0] == "move":
            ready[made] = start + cost
            for zz, extra in ((1, 0.0), (3, 0.0), (2, cost / 3)):
                ready[("hub", step[1], zz)] = start + cost + LAG + extra
        lazy = SLACK if step[0] == "side" and step[1] != (0, 0) else 0.0
        late = 1e4 + 11 if step[:2] == ("line", "o") else 0.0
        steps.append((max(ready[need] + lazy, start - 12.0, late), start, ("send",) + step))
        for kb in ORDER:
            key = ("sum", kb)
            if key not in ready and all(("qs", kb, zz) in ready for zz in range(4)) and ("grad", 2, 1) in ready and (kb > 1 or ("grad", 2, 0) in ready):
                now = max(t for e, t in ready.items() if e[:2] == ("qs", kb) or e[0] == "grad" and (kb < 2 or e[2] == 1)) + 3.0
                ready[key] = now
                steps.append((now, now, ("part", kb)))
                for d in (1, -1):
                    pending.append((key, ("y", d), 5.65, ("hop", kb, d), 0, ("none",)))
                    pending.append((("hop", kb, d), ("y", d), 11.3, ("got", kb, d), 0, ("near", kb, d)))
    for g in range(4):
        steps.append((1e4 + (0, 10, 12, 13)[g], g, ("dot", ("own", "a", "b", "o")[g])))
    steps = [(1e4 + 5, b, s) if s[:3] == ("send", "near", ORDER[-1]) else (a, b, s) for a, b, s in steps]
    steps.sort(key=lambda t: (t[0], t[1]))
    return [s for _, _, s in steps], ready


def kernel(low_ref, side_ref, grad_ref, right_ref, lower_ref, low_all,
           side_all, grad_all, line_all, acc, part, hop, got, lbuf, stage, obuf, rbuf,
           mid, low_recv, side_recv, grad_recv, line_recv, hop_recv, got_recv, mid_recv, send_sem, lbuf_sem, stage_sem, out_sem):
    r, c = lax.axis_index("row"), lax.axis_index("col")
    z, y, x, core = r // 4, r % 4, c // 2, c % 2
    hub = x // 2 == z % 2
    xa, xb = x + 1 - 2 * (x % 2), 3 - x
    xh = jnp.where(hub, x, xb)

    def place(zz, yy, xx, cc):
        return {"row": zz * 4 + yy, "col": xx * 2 + cc}

    def remote(src, dst, send, recv, to):
        return pltpu.make_async_remote_copy(src, dst, send_sem.at[send], recv, device_id=to, device_id_type=MESH)

    def arrive(ref, sem):
        pltpu.make_async_copy(ref, ref, sem).wait()

    sib = place(z, y, x, 1 - core)
    up, down = place(z, (y + 1) % 4, x, core), place(z, (y + 3) % 4, x, core)

    def shift(sig, kk):
        return (sig + kk * (5 - 2 * sig)) % 4

    def spread_row(cj, cc):
        return 2 * shift((cc // 2 + 4 - cj // 2) % 4, cj % 2) + (cj + cc) % 2

    def spread_col(row8, cj):
        return 2 * ((cj // 2 + shift(row8 // 2, cj % 2)) % 4) + (cj + row8) % 2

    def spread_from(row8, cc):
        kk = (cc + row8) % 2
        return 2 * ((cc // 2 + 4 - shift(row8 // 2, kk)) % 4) + kk

    side_row = (r // 8) * 8 + spread_row(c, r % 8)
    side_col = spread_col(r % 8, c)
    stays, direct = side_row == r, c == r % 8

    def quarter(ref, q):
        return ref.at[pl.ds(q * BLOCK, BLOCK)]

    def spread_first():
        @pl.when(jnp.logical_not(stays) & jnp.logical_not(direct))
        def _():
            for q in range(4):
                remote(quarter(side_ref, q), quarter(mid, q), 0, mid_recv.at[q], {"row": side_row, "col": c}).start()

        @pl.when(jnp.logical_not(stays) & direct)
        def _():
            for q in range(4):
                remote(quarter(side_ref, q), quarter(side_all.at[side_row], q), 0, side_recv.at[side_row, q],
                       {"row": side_row, "col": c}).start()

        @pl.when(stays & direct)
        def _():
            for q in range(4):
                pltpu.make_async_copy(quarter(side_ref, q), quarter(side_all.at[r], q), side_recv.at[r, q]).start()

    def spread(q):
        to = {"row": r, "col": side_col}

        @pl.when((side_col != c) & (side_col != r % 8))
        def _():
            arrive(quarter(mid, q), mid_recv.at[q])
            remote(quarter(mid, q), quarter(side_all.at[r], q), 9, side_recv.at[r, q], to).start()

        @pl.when((side_col != c) & (side_col == r % 8))
        def _():
            remote(quarter(side_ref, q), quarter(side_all.at[r], q), 9, side_recv.at[r, q], to).start()

    mine = 2 * (x % 2) + core

    def low_piece(h, kb):
        return low_ref.at[pl.ds(kb * BLOCK, NROWS[kb]), pl.ds(pl.multiple_of((2 * kb + h) * BLOCK, BLOCK), BLOCK)]

    def low_at(yy, zz, kb):
        return low_all.at[yy, zz, pl.ds(FIRST[kb], NROWS[kb])]

    def stage_at(kb):
        return stage.at[pl.ds(FIRST[kb], NROWS[kb])]

    here = z // 2

    @pl.when(hub)
    def _():
        for kb in ORDER:
            pltpu.make_async_copy(low_piece(here, kb), stage_at(kb), stage_sem.at[kb]).start()

    def move(kb):
        @pl.when(hub)
        def _():
            remote(low_piece(1 - here, kb), low_at(mine, z, kb), 1, low_recv.at[mine, z, kb],
                   place((z + 2) % 4, y, x, core)).start()

        @pl.when(jnp.logical_not(hub))
        def _():
            for h in range(2):
                remote(low_piece(h, kb), low_at(mine, z, kb), 1, low_recv.at[mine, z, kb],
                       place(x // 2 + 2 * h, y, x, core)).start()

    move(ORDER[0])
    move(ORDER[1])
    spread_first()

    own_grad = pltpu.make_async_copy(grad_ref, grad_all.at[z], out_sem.at[0])
    own_line = pltpu.make_async_copy(grad_ref, line_all.at[c], out_sem.at[1])
    own_grad.start()
    own_line.start()

    acc[...] = jnp.zeros_like(acc)

    def put_stage(kb):
        @pl.when(hub)
        def _():
            pltpu.make_async_copy(low_piece(here, kb), stage_at(kb), stage_sem.at[kb]).wait()
            pltpu.make_async_copy(stage_at(kb), low_at(mine, z, kb), low_recv.at[mine, z, kb]).start()

    steps, ready = plan()
    waited = set()

    def line_slot(piece):
        xx = {"own": x, "a": xa, "b": xb, "o": (x + 2) % 4}[piece.rstrip("s")]
        return xx * 2 + (1 - core if piece.endswith("s") else core)

    def half_at(ref, slot, half):
        return ref.at[slot, pl.ds(half * 512, 512)]

    def wait(event):
        if event in waited:
            return
        waited.add(event)
        name = event[0]
        if name == "side":
            slot = ((z + event[1][0]) % 4) * 4 + (y + event[1][1]) % 4
            arrive(side_all.at[slot, pl.ds(event[2] * BLOCK, BLOCK)], side_recv.at[slot, event[2]])
        elif name == "grad":
            slot = (z + event[1]) % 4
            arrive(half_at(grad_all, slot, event[2]), grad_recv.at[slot, event[2]])
        elif name == "line":
            slot = line_slot(event[1])
            arrive(half_at(line_all, slot, event[2]), line_recv.at[slot, event[2]])
        else:
            yy = 2 * (xh % 2 if name in ("p", "ps") else 1 - xh % 2) + (1 - core if name.endswith("s") else core)
            zz = (z + event[2]) % 4
            arrive(low_at(yy, zz, event[1]), low_recv.at[yy, zz, event[1]])

    def low_send(yy, zz, kb, send, to):
        remote(low_at(yy, zz, kb), low_at(yy, zz, kb), send, low_recv.at[yy, zz, kb], to).start()

    def send(step):
        name = step[0]
        if name == "spread":
            spread(step[1])
        elif name == "stage":
            put_stage(step[1])
        elif name == "move":
            if step[1] in ORDER[2:] and step[2] == 1:
                move(step[1])
        elif name == "side":
            _, off, q, axis, d = step
            wait(("side", off, q))
            slot = ((z + off[0]) % 4) * 4 + (y + off[1]) % 4
            to = place((z + d + 4) % 4, y, x, core) if axis == 0 else place(z, (y + d + 4) % 4, x, core)
            ref = side_all.at[slot, pl.ds(q * BLOCK, BLOCK)]
            remote(ref, ref, 2, side_recv.at[slot, q], to).start()
        elif name == "grad":
            _, off, half, d = step
            if off:
                wait(("grad", off, half))
            slot = (z + off) % 4
            src = half_at(grad_all, slot, half) if off else grad_ref.at[pl.ds(half * 512, 512)]
            remote(src, half_at(grad_all, slot, half), 3, grad_recv.at[slot, half], place((z + d + 4) % 4, y, x, core)).start()
        elif name == "line":
            _, piece, half, to = step
            if piece != "own":
                wait(("line", piece, half))
            slot = line_slot(piece)
            src = half_at(line_all, slot, half) if piece != "own" else grad_ref.at[pl.ds(half * 512, 512)]
            dest = {"a": place(z, y, xa, core), "b": place(z, y, xb, core), "sib": sib}[to]
            remote(src, half_at(line_all, slot, half), 4, line_recv.at[slot, half], dest).start()
        elif name == "hub":
            _, kb, dz = step
            zz = (z + dz) % 4

            @pl.when(hub)
            def _():
                yy = mine
                arrive(low_at(yy, zz, kb), low_recv.at[yy, zz, kb])
                low_send(yy, zz, kb, 5, place(z, y, xb, core))
                low_send(yy, zz, kb, 5, place(z, y, xa, core))
                low_send(yy, zz, kb, 6, sib)
        elif name == "p":
            _, kb, dz = step
            zz = (z + dz) % 4
            yy = 2 * (xb % 2) + core

            @pl.when(jnp.logical_not(hub))
            def _():
                arrive(low_at(yy, zz, kb), low_recv.at[yy, zz, kb])
                low_send(yy, zz, kb, 5, place(z, y, xa, core))
                low_send(yy, zz, kb, 6, sib)
        elif name == "q":
            _, kb, dz = step
            zz = (z + dz) % 4
            wait(("q", kb, dz))
            low_send(2 * (1 - xh % 2) + core, zz, kb, 6, sib)
        elif name == "far":
            _, kb, d = step
            i = 0 if d == 1 else 1
            rows = pl.ds(i * 128, 128)
            remote(part.at[kb, 0, rows], hop.at[kb, i], 7, hop_recv.at[kb, i], up if d == 1 else down).start()
        elif name == "near":
            _, kb, d = step
            i, t = (0, 3) if d == 1 else (1, 1)
            arrive(hop.at[kb, i], hop_recv.at[kb, i])
            rows = pl.ds(i * 128, 128)
            part[kb, t, rows] += hop[kb, i]
            remote(part.at[kb, t], got.at[kb, i], 8, got_recv.at[kb, i], up if d == 1 else down).start()

    def add_part(kb):
        for zz in range(4):
            for name in ("ps", "q", "qs"):
                wait((name, kb, zz))
        if kb == ORDER[0]:
            own_grad.wait()
        for off in (1, 2, 3):
            for half in (1,) if kb > 1 else (0, 1):
                wait(("grad", off, half))
        n = NROWS[kb]

        def load(t):
            return pltpu.make_async_copy(low_all.at[(y + 2 + t) % 4, :, pl.ds(FIRST[kb], n)],
                                         lbuf.at[t % 2, :, pl.ds(0, n)], lbuf_sem.at[t % 2])

        load(0).start()

        def body(t, carry):
            @pl.when(t < 3)
            def _():
                load(t + 1).start()
            load(t).wait()
            total = jnp.zeros((BLOCK, 512), jnp.float32)
            for zz in range(4):
                total += lax.dot_general(lbuf[t % 2, zz, pl.ds(0, n)], grad_all[zz, pl.ds(kb * BLOCK, n)],
                                         (((0,), (0,)), ((), ())), preferred_element_type=jnp.float32)
            part[kb, t] = total
            return carry

        body(0, 0)
        send(("far", kb, 1))
        send(("far", kb, -1))
        lax.fori_loop(1, 4, body, 0)

    def add_dot(piece, start):
        for name in (piece, piece + "s"):
            if name != "own":
                for half in range(2):
                    wait(("line", name, half))
        if start:
            own_line.wait()
            for a in range(4):
                for b in range(4):
                    for q in range(4):
                        wait(("side", (a, b), q))
        first = line_slot(piece) // 2

        def body(i, carry):
            cj = 2 * first + i % 2
            h = i // 2
            slot = 8 * h + spread_row(cj, c)
            for bi in range(4):
                n = (bi + 1) * BLOCK
                total = lax.dot_general(line_all[cj, bi * BLOCK:(bi + 1) * BLOCK], side_all[slot, :n],
                                        (((1,), (1,)), ((), ())), preferred_element_type=jnp.float32)
                acc[h, bi, :, :n] += total
            return carry

        lax.fori_loop(0, 4, body, 0)

    started = False
    for step in steps:
        if step[0] == "send":
            send(step[1:])
        elif step[0] == "part":
            add_part(step[1])
        else:
            add_dot(step[1], not started)
            started = True

    for bi in range(4):
        if bi >= 2:
            pltpu.make_async_copy(obuf.at[bi % 2], lower_ref.at[pl.ds((bi - 2) * BLOCK, BLOCK)], out_sem.at[2 + bi % 2]).wait()
        for kb in range(4):
            for h in range(2):
                cols = pl.ds((2 * kb + h) * BLOCK, BLOCK)
                if kb <= bi:
                    obuf[bi % 2, :, cols] = acc[h, bi, :, kb * BLOCK:(kb + 1) * BLOCK].astype(jnp.bfloat16)
                else:
                    obuf[bi % 2, :, cols] = jnp.zeros((BLOCK, BLOCK), jnp.bfloat16)
        pltpu.make_async_copy(obuf.at[bi % 2], lower_ref.at[pl.ds(bi * BLOCK, BLOCK)], out_sem.at[2 + bi % 2]).start()
    for kb in range(4):
        for i in range(2):
            arrive(got.at[kb, i], got_recv.at[kb, i])
        rbuf[kb * BLOCK:(kb + 1) * BLOCK] = (part[kb, 2] + got[kb, 0] + got[kb, 1]).astype(jnp.bfloat16)
    out = pltpu.make_async_copy(rbuf, right_ref, out_sem.at[4])
    out.start()

    def sent(ref, i):
        pltpu.make_async_copy(ref, ref, send_sem.at[i]).wait()

    def pieces(n):
        return low_all.at[pl.ds(0, n // 4)] if n >= 4 else low_all.at[0, pl.ds(0, n)]

    @pl.when(jnp.logical_not(stays))
    def _():
        sent(side_all.at[0], 0)

    @pl.when(side_col != c)
    def _():
        sent(side_all.at[0], 9)

    @pl.when(hub)
    def _():
        sent(pieces(1), 1)
        sent(pieces(8), 5)

    @pl.when(jnp.logical_not(hub))
    def _():
        sent(pieces(2), 1)
        sent(pieces(4), 5)

    sent(side_all.at[pl.ds(0, 15)], 2)
    sent(grad_all.at[pl.ds(0, 3)], 3)
    sent(line_all.at[pl.ds(0, 7)], 4)
    sent(pieces(8), 6)
    sent(part.at[:, 0], 7)
    sent(got, 8)
    for bi in (2, 3):
        pltpu.make_async_copy(obuf.at[bi % 2], lower_ref.at[pl.ds(bi * BLOCK, BLOCK)], out_sem.at[2 + bi % 2]).wait()
    out.wait()


def fused(low, side, grad):
    dt = low.dtype
    f32 = jnp.float32
    anywhere = pl.BlockSpec(memory_space=pl.ANY)
    dma = pltpu.SemaphoreType.DMA
    return pl.pallas_call(
        kernel,
        out_shape=[jax.ShapeDtypeStruct(grad.shape, dt), jax.ShapeDtypeStruct(low.shape, dt),
                   jax.ShapeDtypeStruct((4, 4, 2560, BLOCK), dt)],
        in_specs=[anywhere] * 3,
        out_specs=[anywhere] * 3,
        scratch_shapes=[
            pltpu.VMEM((16, 1024, 512), dt),
            pltpu.VMEM((4, 1024, 512), dt),
            pltpu.VMEM((8, 1024, 512), dt),
            pltpu.VMEM((2, 4, BLOCK, 1024), f32),
            pltpu.VMEM((4, 4, BLOCK, 512), f32),
            pltpu.VMEM((4, 2, 128, 512), f32),
            pltpu.VMEM((4, 2, BLOCK, 512), f32),
            pltpu.VMEM((2, 4, 1024, BLOCK), dt),
            pltpu.VMEM((2560, BLOCK), dt),
            pltpu.VMEM((2, BLOCK, 2048), dt),
            pltpu.VMEM((1024, 512), dt),
            pltpu.VMEM((1024, 512), dt),
            dma((4, 4, 4)), dma((16, 4)), dma((4, 2)), dma((8, 2)), dma((4, 2)), dma((4, 2)), dma((4,)),
            dma((10,)), dma((2,)), dma((4,)), dma((5,)),
        ],
        compiler_params=pltpu.CompilerParams(has_side_effects=True, vmem_limit_bytes=67043328),
        name="fused",
    )(low, side, grad)


def per_device(low, side, grad):
    right, lower, _ = fused(low, side, grad)
    row_pos = jnp.arange(lower.shape[0])[:, None]
    col_pos = jnp.arange(lower.shape[1])[None, :]
    row_global = (row_pos // BLOCK * 16 + lax.axis_index("row")) * BLOCK + row_pos % BLOCK
    col_global = (col_pos // BLOCK * 8 + lax.axis_index("col")) * BLOCK + col_pos % BLOCK
    return right, jnp.where(row_global >= col_global, lower, jnp.zeros_like(lower))


def solution(mesh):
    spec = P(("batch", "row"), "col")
    return jax.shard_map(per_device, mesh=mesh, in_specs=(spec,) * 3, out_specs=(spec,) * 2, check_vma=False)
```

```python
import jax
import jax.numpy as jnp
from jax import lax
from jax.experimental import pallas as pl
from jax.experimental.pallas import tpu as pltpu
from jax.sharding import PartitionSpec as P

BLOCK = 256
MESH = pl.DeviceIdType.MESH
NROWS = (1024, 768, 512, 256)
FIRST = (0, 1024, 1792, 2304)
ORDER = (3, 1, 0, 2)
SLACK = 5.0
QROWS = (288, 288, 224, 224)
QFIRST = (0, 288, 576, 800)
LINE = 100.0
LAG = 2.5


def plan():
    ready, jobs, steps = {}, [], []

    def job(need, link, cost, made, prio, step):
        jobs.append((need, link, cost, made, prio, step))

    for q in range(4):
        first = 1 if q < 2 else 0
        cost = 11.3 * QROWS[q] / 512
        def hop(off, axis, d):
            moved = list(off)
            moved[axis] = (moved[axis] - d) % 4
            return tuple(moved)
        ready[("mid", q)] = 16.0 + 8.0 * q
        job(("mid", q), "spread", 8.0, ("side", (0, 0), q), 0, ("spread", q))
        job(("mid", q), "a", 2.8, ("spread a", q), 0, ("none",))
        job(("mid", q), "b", 2.8, ("spread b", q), 0, ("none",))
        for lane in (None, 0, 1, 3, 2):
            axis = first if lane is None else 1 - first
            own = [0, 0]
            if lane is not None:
                own[first] = lane
            own = tuple(own)
            prio = 1 if lane is None else 5
            for d in (1, -1):
                job(("side", own, q), ("zy"[axis], d), cost, ("side", hop(own, axis, d), q), prio, ("side", own, q, axis, d))
            d = 1 if q % 2 == 0 else -1
            near = hop(own, axis, d)
            job(("side", near, q), ("zy"[axis], d), cost, ("side", hop(near, axis, d), q), prio, ("side", near, q, axis, d))
    for half in (1, 0):
        ready[("grad", 0, half)] = 0.0
        ready[("line", "own", half)] = LINE
        for d in (1, -1):
            job(("grad", 0, half), ("z", d), 11.3, ("grad", -d % 4, half), 1.2 if half == 0 else 1, ("grad", 0, half, d))
        d = 1 if half == 0 else -1
        job(("grad", -d % 4, half), ("z", d), 11.3, ("grad", 2, half), 1.2 if half == 0 else 1, ("grad", -d % 4, half, d))
        for to in "ab":
            job(("line", "own", half), to, 11.3, ("line", to, half), 4, ("line", "own", half, to))
        job(("late", "a", half), "b", 11.3, ("line", "o", half), 4, ("line", "a", half, "b"))
        ready[("late", "a", half)] = 130.0
        for piece in ("own", "a", "b", "o"):
            job(("line", piece, half), "sib", 1.0, ("line", piece + "s", half), 4, ("line", piece, half, "sib"))
    ready[("move", ORDER[0])] = 0.0
    ready[("hub", "end", 0)] = 0.0
    for n, kb in enumerate(ORDER):
        cost = 11.3 * NROWS[kb] / 1024
        for d in (1, -1):
            job(("move", kb), ("z", d), 1.5 * cost, ("move", (ORDER + ("end",))[n + 1]) if d == 1 else ("moved", kb), (0, 0, 0.5, 1.5)[n], ("move", kb, d))
        for zz in range(4):
            job(("hub", kb, zz), "b", cost, ("p", kb, zz), 2 + 0.1 * n, ("hub", kb, zz))
            job(("p", kb, zz), "a", cost, ("q", kb, zz), 2 + 0.1 * n, ("p", kb, zz))
            job(("q", kb, zz), "sib", 0.1 * cost, ("qs", kb, zz), 2, ("q", kb, zz))
        ready[("hub", kb, 0)] = 6.0 + 2 * n
        steps.append((2.0 + 2 * n, n, ("send", "stage", kb)))
    steps.append((28.0, 0, ("send", "zero")))
    free = {}
    pending = list(jobs)
    while pending:
        best = min((j for j in pending if j[0] in ready),
                   key=lambda j: (max(ready[j[0]], free.get(j[1], 0.0)), j[4], ready[j[0]]))
        pending.remove(best)
        need, link, cost, made, prio, step = best
        start = max(ready[need], free.get(link, 0.0))
        free[link] = start + cost
        ready[made] = start + cost + LAG
        if made[0] == "move":
            ready[made] = start + cost
            for zz, extra in ((1, 0.0), (3, 0.0), (2, cost / 3)):
                ready[("hub", step[1], zz)] = start + cost + LAG + extra
        lazy = SLACK if step[0] == "side" and step[1] != (0, 0) else 0.0
        late = 0.0
        if step[0] == "line" and step[-1] == "sib":
            late = {"own": 120.0, "o": 1e4 + 11}.get(step[1], 1e4 + 8)
        steps.append((max(ready[need] + lazy, start - 12.0, late), start, ("send",) + step))
        for kb in ORDER:
            key = ("sum", kb)
            if key not in ready and all(("qs", kb, zz) in ready for zz in range(4)) and ("grad", 2, 1) in ready and (kb > 1 or ("grad", 2, 0) in ready):
                now = max(t for e, t in ready.items() if e[:2] == ("qs", kb) or e[0] == "grad" and (kb < 2 or e[2] == 1)) + 3.0
                ready[key] = now
                steps.append((now, now, ("part", kb)))
                for d in (1, -1):
                    pending.append((key, ("y", d), 5.65, ("hop", kb, d), 0, ("none",)))
                    pending.append((("hop", kb, d), ("y", d), 11.3, ("got", kb, d), 0, ("near", kb, d)))
    for g in range(4):
        steps.append((1e4 + (7, 10, 12, 13)[g], g, ("dot", ("own", "a", "b", "o")[g])))
    steps.sort(key=lambda t: (t[0], t[1]))
    return [s for _, _, s in steps], ready


def kernel(low_ref, side_ref, grad_ref, right_ref, lower_ref, low_all,
           side_all, grad_all, line_all, acc, part, hop, got, lbuf, stage, obuf, rbuf,
           mid, low_recv, side_recv, grad_recv, line_recv, hop_recv, got_recv, mid_recv, send_sem, lbuf_sem, stage_sem, out_sem):
    r, c = lax.axis_index("row"), lax.axis_index("col")
    z, y, x, core = r // 4, r % 4, c // 2, c % 2
    hub = x // 2 == z % 2
    xa, xb = x + 1 - 2 * (x % 2), 3 - x
    xh = jnp.where(hub, x, xb)

    def place(zz, yy, xx, cc):
        return {"row": zz * 4 + yy, "col": xx * 2 + cc}

    def remote(src, dst, send, recv, to):
        return pltpu.make_async_remote_copy(src, dst, send_sem.at[send], recv, device_id=to, device_id_type=MESH)

    def arrive(ref, sem):
        pltpu.make_async_copy(ref, ref, sem).wait()

    sib = place(z, y, x, 1 - core)
    up, down = place(z, (y + 1) % 4, x, core), place(z, (y + 3) % 4, x, core)

    def shift(sig, kk):
        return (sig + kk * (5 - 2 * sig)) % 4

    def spread_row(cj, cc):
        return 2 * shift((cc // 2 + 4 - cj // 2) % 4, cj % 2) + (cj + cc) % 2

    def spread_col(row8, cj):
        return 2 * ((cj // 2 + shift(row8 // 2, cj % 2)) % 4) + (cj + row8) % 2

    def spread_from(row8, cc):
        kk = (cc + row8) % 2
        return 2 * ((cc // 2 + 4 - shift(row8 // 2, kk)) % 4) + kk

    side_row = (r // 8) * 8 + spread_row(c, r % 8)
    side_col = spread_col(r % 8, c)
    stays, direct = side_row == r, c == r % 8

    def quarter(ref, q):
        return ref.at[pl.ds(QFIRST[q], QROWS[q])]

    def spread_first():
        @pl.when(jnp.logical_not(stays) & jnp.logical_not(direct))
        def _():
            for q in range(4):
                remote(quarter(side_ref, q), quarter(mid, q), 0, mid_recv.at[q], {"row": side_row, "col": c}).start()

        @pl.when(jnp.logical_not(stays) & direct)
        def _():
            for q in range(4):
                remote(quarter(side_ref, q), quarter(side_all.at[side_row], q), 0, side_recv.at[side_row, q],
                       {"row": side_row, "col": c}).start()

        @pl.when(stays & direct)
        def _():
            for q in range(4):
                pltpu.make_async_copy(quarter(side_ref, q), quarter(side_all.at[r], q), side_recv.at[r, q]).start()

    def spread(q):
        to = {"row": r, "col": side_col}

        @pl.when((side_col != c) & (side_col != r % 8))
        def _():
            arrive(quarter(mid, q), mid_recv.at[q])
            remote(quarter(mid, q), quarter(side_all.at[r], q), 9, side_recv.at[r, q], to).start()

        @pl.when((side_col != c) & (side_col == r % 8))
        def _():
            remote(quarter(side_ref, q), quarter(side_all.at[r], q), 9, side_recv.at[r, q], to).start()

    mine = 2 * (x % 2) + core

    def low_piece(h, kb):
        return low_ref.at[pl.ds(kb * BLOCK, NROWS[kb]), pl.ds(pl.multiple_of((2 * kb + h) * BLOCK, BLOCK), BLOCK)]

    def low_at(yy, zz, kb):
        return low_all.at[yy, zz, pl.ds(FIRST[kb], NROWS[kb])]

    def stage_at(kb):
        return stage.at[pl.ds(FIRST[kb], NROWS[kb])]

    here = z // 2

    @pl.when(hub)
    def _():
        for kb in ORDER:
            pltpu.make_async_copy(low_piece(here, kb), stage_at(kb), stage_sem.at[kb]).start()

    def move(kb):
        @pl.when(hub)
        def _():
            remote(low_piece(1 - here, kb), low_at(mine, z, kb), 1, low_recv.at[mine, z, kb],
                   place((z + 2) % 4, y, x, core)).start()

        @pl.when(jnp.logical_not(hub))
        def _():
            for h in range(2):
                remote(low_piece(h, kb), low_at(mine, z, kb), 1, low_recv.at[mine, z, kb],
                       place(x // 2 + 2 * h, y, x, core)).start()

    move(ORDER[0])
    move(ORDER[1])
    spread_first()

    own_grad = pltpu.make_async_copy(grad_ref, grad_all.at[z], out_sem.at[0])
    own_line = pltpu.make_async_copy(grad_ref, line_all.at[c], out_sem.at[1])
    own_grad.start()
    own_line.start()

    def put_stage(kb):
        @pl.when(hub)
        def _():
            pltpu.make_async_copy(low_piece(here, kb), stage_at(kb), stage_sem.at[kb]).wait()
            pltpu.make_async_copy(stage_at(kb), low_at(mine, z, kb), low_recv.at[mine, z, kb]).start()

    steps, ready = plan()
    waited = set()

    def line_slot(piece):
        xx = {"own": x, "a": xa, "b": xb, "o": (x + 2) % 4}[piece.rstrip("s")]
        return xx * 2 + (1 - core if piece.endswith("s") else core)

    def half_at(ref, slot, half):
        return ref.at[slot, pl.ds(half * 512, 512)]

    def wait(event):
        if event in waited:
            return
        waited.add(event)
        name = event[0]
        if name == "side":
            slot = ((z + event[1][0]) % 4) * 4 + (y + event[1][1]) % 4
            arrive(quarter(side_all.at[slot], event[2]), side_recv.at[slot, event[2]])
        elif name == "grad":
            slot = (z + event[1]) % 4
            arrive(half_at(grad_all, slot, event[2]), grad_recv.at[slot, event[2]])
        elif name == "line":
            slot = line_slot(event[1])
            arrive(half_at(line_all, slot, event[2]), line_recv.at[slot, event[2]])
        else:
            yy = 2 * (xh % 2 if name in ("p", "ps") else 1 - xh % 2) + (1 - core if name.endswith("s") else core)
            zz = (z + event[2]) % 4
            arrive(low_at(yy, zz, event[1]), low_recv.at[yy, zz, event[1]])

    def low_send(yy, zz, kb, send, to):
        remote(low_at(yy, zz, kb), low_at(yy, zz, kb), send, low_recv.at[yy, zz, kb], to).start()

    def send(step):
        name = step[0]
        if name == "spread":
            spread(step[1])
        elif name == "stage":
            put_stage(step[1])
        elif name == "zero":
            acc[...] = jnp.zeros_like(acc)
        elif name == "move":
            if step[1] in ORDER[2:] and step[2] == 1:
                move(step[1])
        elif name == "side":
            _, off, q, axis, d = step
            wait(("side", off, q))
            slot = ((z + off[0]) % 4) * 4 + (y + off[1]) % 4
            to = place((z + d + 4) % 4, y, x, core) if axis == 0 else place(z, (y + d + 4) % 4, x, core)
            ref = quarter(side_all.at[slot], q)
            remote(ref, ref, 2, side_recv.at[slot, q], to).start()
        elif name == "grad":
            _, off, half, d = step
            if off:
                wait(("grad", off, half))
            slot = (z + off) % 4
            src = half_at(grad_all, slot, half) if off else grad_ref.at[pl.ds(half * 512, 512)]
            remote(src, half_at(grad_all, slot, half), 3, grad_recv.at[slot, half], place((z + d + 4) % 4, y, x, core)).start()
        elif name == "line":
            _, piece, half, to = step
            if piece != "own":
                wait(("line", piece, half))
            slot = line_slot(piece)
            src = half_at(line_all, slot, half) if piece != "own" else grad_ref.at[pl.ds(half * 512, 512)]
            dest = {"a": place(z, y, xa, core), "b": place(z, y, xb, core), "sib": sib}[to]
            remote(src, half_at(line_all, slot, half), 4, line_recv.at[slot, half], dest).start()
        elif name == "hub":
            _, kb, dz = step
            zz = (z + dz) % 4

            @pl.when(hub)
            def _():
                yy = mine
                arrive(low_at(yy, zz, kb), low_recv.at[yy, zz, kb])
                low_send(yy, zz, kb, 5, place(z, y, xb, core))
                low_send(yy, zz, kb, 5, place(z, y, xa, core))
                low_send(yy, zz, kb, 6, sib)
        elif name == "p":
            _, kb, dz = step
            zz = (z + dz) % 4
            yy = 2 * (xb % 2) + core

            @pl.when(jnp.logical_not(hub))
            def _():
                arrive(low_at(yy, zz, kb), low_recv.at[yy, zz, kb])
                low_send(yy, zz, kb, 5, place(z, y, xa, core))
                low_send(yy, zz, kb, 6, sib)
        elif name == "q":
            _, kb, dz = step
            zz = (z + dz) % 4
            wait(("q", kb, dz))
            low_send(2 * (1 - xh % 2) + core, zz, kb, 6, sib)
        elif name == "far":
            _, kb, d = step
            i = 0 if d == 1 else 1
            rows = pl.ds(i * 128, 128)
            remote(part.at[kb, 0, rows], hop.at[kb, i], 7, hop_recv.at[kb, i], up if d == 1 else down).start()
        elif name == "near":
            _, kb, d = step
            i, t = (0, 3) if d == 1 else (1, 1)
            arrive(hop.at[kb, i], hop_recv.at[kb, i])
            rows = pl.ds(i * 128, 128)
            part[kb, t, rows] += hop[kb, i]
            remote(part.at[kb, t], got.at[kb, i], 8, got_recv.at[kb, i], up if d == 1 else down).start()

    def add_part(kb):
        for zz in range(4):
            for name in ("ps", "q", "qs"):
                wait((name, kb, zz))
        if kb == ORDER[0]:
            own_grad.wait()
        for off in (1, 2, 3):
            for half in (1,) if kb > 1 else (0, 1):
                wait(("grad", off, half))
        n = NROWS[kb]

        def load(t):
            return pltpu.make_async_copy(low_all.at[(y + 2 + t) % 4, :, pl.ds(FIRST[kb], n)],
                                         lbuf.at[t % 2, :, pl.ds(0, n)], lbuf_sem.at[t % 2])

        load(0).start()

        def body(t, carry):
            @pl.when(t < 3)
            def _():
                load(t + 1).start()
            load(t).wait()
            total = jnp.zeros((BLOCK, 512), jnp.float32)
            for zz in range(4):
                total += lax.dot_general(lbuf[t % 2, zz, pl.ds(0, n)], grad_all[zz, pl.ds(kb * BLOCK, n)],
                                         (((0,), (0,)), ((), ())), preferred_element_type=jnp.float32)
            part[kb, t] = total
            return carry

        body(0, 0)
        send(("far", kb, 1))
        send(("far", kb, -1))
        lax.fori_loop(1, 4, body, 0)

    def add_dot(piece, start):
        for name in (piece, piece + "s"):
            if name != "own":
                for half in range(2):
                    wait(("line", name, half))
        if start:
            own_line.wait()
            for a in range(4):
                for b in range(4):
                    for q in range(4):
                        wait(("side", (a, b), q))
        first = line_slot(piece) // 2

        def body(i, carry):
            cj = 2 * first + i % 2
            h = i // 2
            slot = 8 * h + spread_row(cj, c)
            for bi in range(4):
                n = (bi + 1) * BLOCK
                total = lax.dot_general(line_all[cj, bi * BLOCK:(bi + 1) * BLOCK], side_all[slot, :n],
                                        (((1,), (1,)), ((), ())), preferred_element_type=jnp.float32)
                acc[h, bi, :, :n] += total
            return carry

        lax.fori_loop(0, 4, body, 0)

    started = False
    for step in steps:
        if step[0] == "send":
            send(step[1:])
        elif step[0] == "part":
            add_part(step[1])
        else:
            add_dot(step[1], not started)
            started = True

    for bi in range(4):
        if bi >= 2:
            pltpu.make_async_copy(obuf.at[bi % 2], lower_ref.at[pl.ds((bi - 2) * BLOCK, BLOCK)], out_sem.at[2 + bi % 2]).wait()
        for kb in range(4):
            for h in range(2):
                cols = pl.ds((2 * kb + h) * BLOCK, BLOCK)
                if kb <= bi:
                    obuf[bi % 2, :, cols] = acc[h, bi, :, kb * BLOCK:(kb + 1) * BLOCK].astype(jnp.bfloat16)
                else:
                    obuf[bi % 2, :, cols] = jnp.zeros((BLOCK, BLOCK), jnp.bfloat16)
        pltpu.make_async_copy(obuf.at[bi % 2], lower_ref.at[pl.ds(bi * BLOCK, BLOCK)], out_sem.at[2 + bi % 2]).start()
    for kb in range(4):
        for i in range(2):
            arrive(got.at[kb, i], got_recv.at[kb, i])
        rbuf[kb * BLOCK:(kb + 1) * BLOCK] = (part[kb, 2] + got[kb, 0] + got[kb, 1]).astype(jnp.bfloat16)
    out = pltpu.make_async_copy(rbuf, right_ref, out_sem.at[4])
    out.start()

    def sent(ref, i):
        pltpu.make_async_copy(ref, ref, send_sem.at[i]).wait()

    def pieces(n):
        return low_all.at[pl.ds(0, n // 4)] if n >= 4 else low_all.at[0, pl.ds(0, n)]

    @pl.when(jnp.logical_not(stays))
    def _():
        sent(side_all.at[0], 0)

    @pl.when(side_col != c)
    def _():
        sent(side_all.at[0], 9)

    @pl.when(hub)
    def _():
        sent(pieces(1), 1)
        sent(pieces(8), 5)

    @pl.when(jnp.logical_not(hub))
    def _():
        sent(pieces(2), 1)
        sent(pieces(4), 5)

    sent(side_all.at[pl.ds(0, 15)], 2)
    sent(grad_all.at[pl.ds(0, 3)], 3)
    sent(line_all.at[pl.ds(0, 7)], 4)
    sent(pieces(8), 6)
    sent(part.at[:, 0], 7)
    sent(got, 8)
    for bi in (2, 3):
        pltpu.make_async_copy(obuf.at[bi % 2], lower_ref.at[pl.ds(bi * BLOCK, BLOCK)], out_sem.at[2 + bi % 2]).wait()
    out.wait()


def fused(low, side, grad):
    dt = low.dtype
    f32 = jnp.float32
    anywhere = pl.BlockSpec(memory_space=pl.ANY)
    dma = pltpu.SemaphoreType.DMA
    return pl.pallas_call(
        kernel,
        out_shape=[jax.ShapeDtypeStruct(grad.shape, dt), jax.ShapeDtypeStruct(low.shape, dt),
                   jax.ShapeDtypeStruct((4, 4, 2560, BLOCK), dt)],
        in_specs=[anywhere] * 3,
        out_specs=[anywhere] * 3,
        scratch_shapes=[
            pltpu.VMEM((16, 1024, 512), dt),
            pltpu.VMEM((4, 1024, 512), dt),
            pltpu.VMEM((8, 1024, 512), dt),
            pltpu.VMEM((2, 4, BLOCK, 1024), f32),
            pltpu.VMEM((4, 4, BLOCK, 512), f32),
            pltpu.VMEM((4, 2, 128, 512), f32),
            pltpu.VMEM((4, 2, BLOCK, 512), f32),
            pltpu.VMEM((2, 4, 1024, BLOCK), dt),
            pltpu.VMEM((2560, BLOCK), dt),
            pltpu.VMEM((2, BLOCK, 2048), dt),
            pltpu.VMEM((1024, 512), dt),
            pltpu.VMEM((1024, 512), dt),
            dma((4, 4, 4)), dma((16, 4)), dma((4, 2)), dma((8, 2)), dma((4, 2)), dma((4, 2)), dma((4,)),
            dma((10,)), dma((2,)), dma((4,)), dma((5,)),
        ],
        compiler_params=pltpu.CompilerParams(has_side_effects=True, vmem_limit_bytes=67043328),
        name="fused",
    )(low, side, grad)


def per_device(low, side, grad):
    right, lower, _ = fused(low, side, grad)
    row_pos = jnp.arange(lower.shape[0])[:, None]
    col_pos = jnp.arange(lower.shape[1])[None, :]
    row_global = (row_pos // BLOCK * 16 + lax.axis_index("row")) * BLOCK + row_pos % BLOCK
    col_global = (col_pos // BLOCK * 8 + lax.axis_index("col")) * BLOCK + col_pos % BLOCK
    return right, jnp.where(row_global >= col_global, lower, jnp.zeros_like(lower))


def solution(mesh):
    spec = P(("batch", "row"), "col")
    return jax.shard_map(per_device, mesh=mesh, in_specs=(spec,) * 3, out_specs=(spec,) * 2, check_vma=False)
```

```python
import jax
import jax.numpy as jnp
from jax import lax
from jax.experimental import pallas as pl
from jax.experimental.pallas import tpu as pltpu
from jax.sharding import PartitionSpec as P

BLOCK = 256
MESH = pl.DeviceIdType.MESH
NROWS = (1024, 768, 512, 256)
FIRST = (0, 1024, 1792, 2304)
ORDER = (3, 1, 0, 2)
SLACK = 5.0
QROWS = (288, 288, 224, 224)
QFIRST = (0, 288, 576, 800)
LINE = (110.0, 0.0)
LAG = 2.5


def plan():
    ready, jobs, steps = {}, [], []

    def job(need, link, cost, made, prio, step):
        jobs.append((need, link, cost, made, prio, step))

    for q in range(4):
        first = 1 if q < 2 else 0
        cost = 11.3 * QROWS[q] / 512
        def hop(off, axis, d):
            moved = list(off)
            moved[axis] = (moved[axis] - d) % 4
            return tuple(moved)
        ready[("mid", q)] = 16.0 + 8.0 * q
        job(("mid", q), "spread", 8.0, ("side", (0, 0), q), 0, ("spread", q))
        job(("mid", q), "a", 2.8, ("spread a", q), 0, ("none",))
        job(("mid", q), "b", 2.8, ("spread b", q), 0, ("none",))
        for lane in (None, 0, 1, 3, 2):
            axis = first if lane is None else 1 - first
            own = [0, 0]
            if lane is not None:
                own[first] = lane
            own = tuple(own)
            prio = 1 if lane is None else 5
            for d in (1, -1):
                job(("side", own, q), ("zy"[axis], d), cost, ("side", hop(own, axis, d), q), prio, ("side", own, q, axis, d))
            d = 1 if q % 2 == 0 else -1
            near = hop(own, axis, d)
            job(("side", near, q), ("zy"[axis], d), cost, ("side", hop(near, axis, d), q), prio, ("side", near, q, axis, d))
    for half in (1, 0):
        ready[("grad", 0, half)] = 0.0
        ready[("line", "own", half)] = LINE[half]
        for d in (1, -1):
            job(("grad", 0, half), ("z", d), 11.3, ("grad", -d % 4, half), 1.2 if half == 0 else 1, ("grad", 0, half, d))
        d = 1 if half == 0 else -1
        job(("grad", -d % 4, half), ("z", d), 11.3, ("grad", 2, half), 1.2 if half == 0 else 1, ("grad", -d % 4, half, d))
        for to in "ab":
            job(("line", "own", half), to, 11.3, ("line", to, half), 4, ("line", "own", half, to))
        job(("late", "a", half), "b", 11.3, ("line", "o", half), 4, ("line", "a", half, "b"))
        ready[("late", "a", half)] = 130.0 - 15.0 * half
        for piece in ("own", "a", "b", "o"):
            job(("line", piece, half), "sib", 1.0, ("line", piece + "s", half), 4, ("line", piece, half, "sib"))
    ready[("move", ORDER[0])] = 0.0
    ready[("hub", "end", 0)] = 0.0
    for n, kb in enumerate(ORDER):
        cost = 11.3 * NROWS[kb] / 1024
        for d in (1, -1):
            job(("move", kb), ("z", d), 1.5 * cost, ("move", (ORDER + ("end",))[n + 1]) if d == 1 else ("moved", kb), (0, 0, 0.5, 1.5)[n], ("move", kb, d))
        for zz in range(4):
            job(("hub", kb, zz), "b", cost, ("p", kb, zz), 2 + 0.1 * n, ("hub", kb, zz))
            job(("p", kb, zz), "a", cost, ("q", kb, zz), 2 + 0.1 * n, ("p", kb, zz))
            job(("q", kb, zz), "sib", 0.1 * cost, ("qs", kb, zz), 2, ("q", kb, zz))
        ready[("hub", kb, 0)] = 6.0 + 2 * n
        steps.append((2.0 + 2 * n, n, ("send", "stage", kb)))
    steps.append((28.0, 0, ("send", "zero")))
    free = {}
    pending = list(jobs)
    while pending:
        best = min((j for j in pending if j[0] in ready),
                   key=lambda j: (max(ready[j[0]], free.get(j[1], 0.0)), j[4], ready[j[0]]))
        pending.remove(best)
        need, link, cost, made, prio, step = best
        start = max(ready[need], free.get(link, 0.0))
        free[link] = start + cost
        ready[made] = start + cost + LAG
        if made[0] == "move":
            ready[made] = start + cost
            for zz, extra in ((1, 0.0), (3, 0.0), (2, cost / 3)):
                ready[("hub", step[1], zz)] = start + cost + LAG + extra
        lazy = SLACK if step[0] == "side" and step[1] != (0, 0) else 0.0
        late = 1e4 + 1 if step == ("line", "a", 0, "b") else 0.0
        if step[0] == "line" and step[-1] == "sib":
            late = {"own": 120.0, "o": 1e4 + 11}.get(step[1], 1e4 + 8)
        steps.append((max(ready[need] + lazy, start - 12.0, late), start, ("send",) + step))
        for kb in ORDER:
            key = ("sum", kb)
            if key not in ready and all(("qs", kb, zz) in ready for zz in range(4)) and ("grad", 2, 1) in ready and (kb > 1 or ("grad", 2, 0) in ready):
                now = max(t for e, t in ready.items() if e[:2] == ("qs", kb) or e[0] == "grad" and (kb < 2 or e[2] == 1)) + 3.0
                ready[key] = now
                steps.append((now, now, ("part", kb)))
                for d in (1, -1):
                    pending.append((key, ("y", d), 5.65, ("hop", kb, d), 0, ("none",)))
                    pending.append((("hop", kb, d), ("y", d), 11.3, ("got", kb, d), 0, ("near", kb, d)))
    for g in range(4):
        steps.append((1e4 + (7, 10, 12, 13)[g], g, ("dot", ("own", "a", "b", "o")[g])))
    steps.sort(key=lambda t: (t[0], t[1]))
    return [s for _, _, s in steps], ready


def kernel(low_ref, side_ref, grad_ref, right_ref, lower_ref, low_all,
           side_all, grad_all, line_all, acc, part, hop, got, lbuf, stage, obuf, rbuf,
           mid, low_recv, side_recv, grad_recv, line_recv, hop_recv, got_recv, mid_recv, send_sem, lbuf_sem, stage_sem, out_sem):
    r, c = lax.axis_index("row"), lax.axis_index("col")
    z, y, x, core = r // 4, r % 4, c // 2, c % 2
    hub = x // 2 == z % 2
    xa, xb = x + 1 - 2 * (x % 2), 3 - x
    xh = jnp.where(hub, x, xb)

    def place(zz, yy, xx, cc):
        return {"row": zz * 4 + yy, "col": xx * 2 + cc}

    def remote(src, dst, send, recv, to):
        return pltpu.make_async_remote_copy(src, dst, send_sem.at[send], recv, device_id=to, device_id_type=MESH)

    def arrive(ref, sem):
        pltpu.make_async_copy(ref, ref, sem).wait()

    sib = place(z, y, x, 1 - core)
    up, down = place(z, (y + 1) % 4, x, core), place(z, (y + 3) % 4, x, core)

    def shift(sig, kk):
        return (sig + kk * (5 - 2 * sig)) % 4

    def spread_row(cj, cc):
        return 2 * shift((cc // 2 + 4 - cj // 2) % 4, cj % 2) + (cj + cc) % 2

    def spread_col(row8, cj):
        return 2 * ((cj // 2 + shift(row8 // 2, cj % 2)) % 4) + (cj + row8) % 2

    def spread_from(row8, cc):
        kk = (cc + row8) % 2
        return 2 * ((cc // 2 + 4 - shift(row8 // 2, kk)) % 4) + kk

    side_row = (r // 8) * 8 + spread_row(c, r % 8)
    side_col = spread_col(r % 8, c)
    stays, direct = side_row == r, c == r % 8

    def quarter(ref, q):
        return ref.at[pl.ds(QFIRST[q], QROWS[q])]

    def spread_first():
        @pl.when(jnp.logical_not(stays) & jnp.logical_not(direct))
        def _():
            for q in range(4):
                remote(quarter(side_ref, q), quarter(mid, q), 0, mid_recv.at[q], {"row": side_row, "col": c}).start()

        @pl.when(jnp.logical_not(stays) & direct)
        def _():
            for q in range(4):
                remote(quarter(side_ref, q), quarter(side_all.at[side_row], q), 0, side_recv.at[side_row, q],
                       {"row": side_row, "col": c}).start()

        @pl.when(stays & direct)
        def _():
            for q in range(4):
                pltpu.make_async_copy(quarter(side_ref, q), quarter(side_all.at[r], q), side_recv.at[r, q]).start()

    def spread(q):
        to = {"row": r, "col": side_col}

        @pl.when((side_col != c) & (side_col != r % 8))
        def _():
            arrive(quarter(mid, q), mid_recv.at[q])
            remote(quarter(mid, q), quarter(side_all.at[r], q), 9, side_recv.at[r, q], to).start()

        @pl.when((side_col != c) & (side_col == r % 8))
        def _():
            remote(quarter(side_ref, q), quarter(side_all.at[r], q), 9, side_recv.at[r, q], to).start()

    mine = 2 * (x % 2) + core

    def low_piece(h, kb):
        return low_ref.at[pl.ds(kb * BLOCK, NROWS[kb]), pl.ds(pl.multiple_of((2 * kb + h) * BLOCK, BLOCK), BLOCK)]

    def low_at(yy, zz, kb):
        return low_all.at[yy, zz, pl.ds(FIRST[kb], NROWS[kb])]

    def stage_at(kb):
        return stage.at[pl.ds(FIRST[kb], NROWS[kb])]

    here = z // 2

    @pl.when(hub)
    def _():
        for kb in ORDER:
            pltpu.make_async_copy(low_piece(here, kb), stage_at(kb), stage_sem.at[kb]).start()

    def move(kb):
        @pl.when(hub)
        def _():
            remote(low_piece(1 - here, kb), low_at(mine, z, kb), 1, low_recv.at[mine, z, kb],
                   place((z + 2) % 4, y, x, core)).start()

        @pl.when(jnp.logical_not(hub))
        def _():
            for h in range(2):
                remote(low_piece(h, kb), low_at(mine, z, kb), 1, low_recv.at[mine, z, kb],
                       place(x // 2 + 2 * h, y, x, core)).start()

    move(ORDER[0])
    move(ORDER[1])
    spread_first()

    own_grad = pltpu.make_async_copy(grad_ref, grad_all.at[z], out_sem.at[0])
    own_line = pltpu.make_async_copy(grad_ref, line_all.at[c], out_sem.at[1])
    own_grad.start()
    own_line.start()

    def put_stage(kb):
        @pl.when(hub)
        def _():
            pltpu.make_async_copy(low_piece(here, kb), stage_at(kb), stage_sem.at[kb]).wait()
            pltpu.make_async_copy(stage_at(kb), low_at(mine, z, kb), low_recv.at[mine, z, kb]).start()

    steps, ready = plan()
    waited = set()

    def line_slot(piece):
        xx = {"own": x, "a": xa, "b": xb, "o": (x + 2) % 4}[piece.rstrip("s")]
        return xx * 2 + (1 - core if piece.endswith("s") else core)

    def half_at(ref, slot, half):
        return ref.at[slot, pl.ds(half * 512, 512)]

    def wait(event):
        if event in waited:
            return
        waited.add(event)
        name = event[0]
        if name == "side":
            slot = ((z + event[1][0]) % 4) * 4 + (y + event[1][1]) % 4
            arrive(quarter(side_all.at[slot], event[2]), side_recv.at[slot, event[2]])
        elif name == "grad":
            slot = (z + event[1]) % 4
            arrive(half_at(grad_all, slot, event[2]), grad_recv.at[slot, event[2]])
        elif name == "line":
            slot = line_slot(event[1])
            arrive(half_at(line_all, slot, event[2]), line_recv.at[slot, event[2]])
        else:
            yy = 2 * (xh % 2 if name in ("p", "ps") else 1 - xh % 2) + (1 - core if name.endswith("s") else core)
            zz = (z + event[2]) % 4
            arrive(low_at(yy, zz, event[1]), low_recv.at[yy, zz, event[1]])

    def low_send(yy, zz, kb, send, to):
        remote(low_at(yy, zz, kb), low_at(yy, zz, kb), send, low_recv.at[yy, zz, kb], to).start()

    def send(step):
        name = step[0]
        if name == "spread":
            spread(step[1])
        elif name == "stage":
            put_stage(step[1])
        elif name == "zero":
            acc[...] = jnp.zeros_like(acc)
        elif name == "move":
            if step[1] in ORDER[2:] and step[2] == 1:
                move(step[1])
        elif name == "side":
            _, off, q, axis, d = step
            wait(("side", off, q))
            slot = ((z + off[0]) % 4) * 4 + (y + off[1]) % 4
            to = place((z + d + 4) % 4, y, x, core) if axis == 0 else place(z, (y + d + 4) % 4, x, core)
            ref = quarter(side_all.at[slot], q)
            remote(ref, ref, 2, side_recv.at[slot, q], to).start()
        elif name == "grad":
            _, off, half, d = step
            if off:
                wait(("grad", off, half))
            slot = (z + off) % 4
            src = half_at(grad_all, slot, half) if off else grad_ref.at[pl.ds(half * 512, 512)]
            remote(src, half_at(grad_all, slot, half), 3, grad_recv.at[slot, half], place((z + d + 4) % 4, y, x, core)).start()
        elif name == "line":
            _, piece, half, to = step
            if piece != "own":
                wait(("line", piece, half))
            slot = line_slot(piece)
            src = half_at(line_all, slot, half) if piece != "own" else grad_ref.at[pl.ds(half * 512, 512)]
            dest = {"a": place(z, y, xa, core), "b": place(z, y, xb, core), "sib": sib}[to]
            remote(src, half_at(line_all, slot, half), 4, line_recv.at[slot, half], dest).start()
        elif name == "hub":
            _, kb, dz = step
            zz = (z + dz) % 4

            @pl.when(hub)
            def _():
                yy = mine
                arrive(low_at(yy, zz, kb), low_recv.at[yy, zz, kb])
                low_send(yy, zz, kb, 5, place(z, y, xb, core))
                low_send(yy, zz, kb, 5, place(z, y, xa, core))
                low_send(yy, zz, kb, 6, sib)
        elif name == "p":
            _, kb, dz = step
            zz = (z + dz) % 4
            yy = 2 * (xb % 2) + core

            @pl.when(jnp.logical_not(hub))
            def _():
                arrive(low_at(yy, zz, kb), low_recv.at[yy, zz, kb])
                low_send(yy, zz, kb, 5, place(z, y, xa, core))
                low_send(yy, zz, kb, 6, sib)
        elif name == "q":
            _, kb, dz = step
            zz = (z + dz) % 4
            wait(("q", kb, dz))
            low_send(2 * (1 - xh % 2) + core, zz, kb, 6, sib)
        elif name == "far":
            _, kb, d = step
            i = 0 if d == 1 else 1
            rows = pl.ds(i * 128, 128)
            remote(part.at[kb, 0, rows], hop.at[kb, i], 7, hop_recv.at[kb, i], up if d == 1 else down).start()
        elif name == "near":
            _, kb, d = step
            i, t = (0, 3) if d == 1 else (1, 1)
            arrive(hop.at[kb, i], hop_recv.at[kb, i])
            rows = pl.ds(i * 128, 128)
            part[kb, t, rows] += hop[kb, i]
            remote(part.at[kb, t], got.at[kb, i], 8, got_recv.at[kb, i], up if d == 1 else down).start()

    def add_part(kb):
        for zz in range(4):
            for name in ("ps", "q", "qs"):
                wait((name, kb, zz))
        if kb == ORDER[0]:
            own_grad.wait()
        for off in (1, 2, 3):
            for half in (1,) if kb > 1 else (0, 1):
                wait(("grad", off, half))
        n = NROWS[kb]

        def load(t):
            return pltpu.make_async_copy(low_all.at[(y + 2 + t) % 4, :, pl.ds(FIRST[kb], n)],
                                         lbuf.at[t % 2, :, pl.ds(0, n)], lbuf_sem.at[t % 2])

        load(0).start()

        def body(t, carry):
            @pl.when(t < 3)
            def _():
                load(t + 1).start()
            load(t).wait()
            total = jnp.zeros((BLOCK, 512), jnp.float32)
            for zz in range(4):
                total += lax.dot_general(lbuf[t % 2, zz, pl.ds(0, n)], grad_all[zz, pl.ds(kb * BLOCK, n)],
                                         (((0,), (0,)), ((), ())), preferred_element_type=jnp.float32)
            part[kb, t] = total
            return carry

        body(0, 0)
        send(("far", kb, 1))
        send(("far", kb, -1))
        lax.fori_loop(1, 4, body, 0)

    def add_dot(piece, start):
        for name in (piece, piece + "s"):
            if name != "own":
                for half in range(2):
                    wait(("line", name, half))
        if start:
            own_line.wait()
            for a in range(4):
                for b in range(4):
                    for q in range(4):
                        wait(("side", (a, b), q))
        first = line_slot(piece) // 2

        def body(i, carry):
            cj = 2 * first + i % 2
            h = i // 2
            slot = 8 * h + spread_row(cj, c)
            for bi in range(4):
                n = (bi + 1) * BLOCK
                total = lax.dot_general(line_all[cj, bi * BLOCK:(bi + 1) * BLOCK], side_all[slot, :n],
                                        (((1,), (1,)), ((), ())), preferred_element_type=jnp.float32)
                acc[h, bi, :, :n] += total
            return carry

        lax.fori_loop(0, 4, body, 0)

    started = False
    for step in steps:
        if step[0] == "send":
            send(step[1:])
        elif step[0] == "part":
            add_part(step[1])
        else:
            add_dot(step[1], not started)
            started = True

    for bi in range(4):
        if bi >= 2:
            pltpu.make_async_copy(obuf.at[bi % 2], lower_ref.at[pl.ds((bi - 2) * BLOCK, BLOCK)], out_sem.at[2 + bi % 2]).wait()
        for kb in range(4):
            for h in range(2):
                cols = pl.ds((2 * kb + h) * BLOCK, BLOCK)
                if kb <= bi:
                    obuf[bi % 2, :, cols] = acc[h, bi, :, kb * BLOCK:(kb + 1) * BLOCK].astype(jnp.bfloat16)
                else:
                    obuf[bi % 2, :, cols] = jnp.zeros((BLOCK, BLOCK), jnp.bfloat16)
        pltpu.make_async_copy(obuf.at[bi % 2], lower_ref.at[pl.ds(bi * BLOCK, BLOCK)], out_sem.at[2 + bi % 2]).start()
    for kb in range(4):
        for i in range(2):
            arrive(got.at[kb, i], got_recv.at[kb, i])
        rbuf[kb * BLOCK:(kb + 1) * BLOCK] = (part[kb, 2] + got[kb, 0] + got[kb, 1]).astype(jnp.bfloat16)
    out = pltpu.make_async_copy(rbuf, right_ref, out_sem.at[4])
    out.start()

    def sent(ref, i):
        pltpu.make_async_copy(ref, ref, send_sem.at[i]).wait()

    def pieces(n):
        return low_all.at[pl.ds(0, n // 4)] if n >= 4 else low_all.at[0, pl.ds(0, n)]

    @pl.when(jnp.logical_not(stays))
    def _():
        sent(side_all.at[0], 0)

    @pl.when(side_col != c)
    def _():
        sent(side_all.at[0], 9)

    @pl.when(hub)
    def _():
        sent(pieces(1), 1)
        sent(pieces(8), 5)

    @pl.when(jnp.logical_not(hub))
    def _():
        sent(pieces(2), 1)
        sent(pieces(4), 5)

    sent(side_all.at[pl.ds(0, 15)], 2)
    sent(grad_all.at[pl.ds(0, 3)], 3)
    sent(line_all.at[pl.ds(0, 7)], 4)
    sent(pieces(8), 6)
    sent(part.at[:, 0], 7)
    sent(got, 8)
    for bi in (2, 3):
        pltpu.make_async_copy(obuf.at[bi % 2], lower_ref.at[pl.ds(bi * BLOCK, BLOCK)], out_sem.at[2 + bi % 2]).wait()
    out.wait()


def fused(low, side, grad):
    dt = low.dtype
    f32 = jnp.float32
    anywhere = pl.BlockSpec(memory_space=pl.ANY)
    dma = pltpu.SemaphoreType.DMA
    return pl.pallas_call(
        kernel,
        out_shape=[jax.ShapeDtypeStruct(grad.shape, dt), jax.ShapeDtypeStruct(low.shape, dt),
                   jax.ShapeDtypeStruct((4, 4, 2560, BLOCK), dt)],
        in_specs=[anywhere] * 3,
        out_specs=[anywhere] * 3,
        scratch_shapes=[
            pltpu.VMEM((16, 1024, 512), dt),
            pltpu.VMEM((4, 1024, 512), dt),
            pltpu.VMEM((8, 1024, 512), dt),
            pltpu.VMEM((2, 4, BLOCK, 1024), f32),
            pltpu.VMEM((4, 4, BLOCK, 512), f32),
            pltpu.VMEM((4, 2, 128, 512), f32),
            pltpu.VMEM((4, 2, BLOCK, 512), f32),
            pltpu.VMEM((2, 4, 1024, BLOCK), dt),
            pltpu.VMEM((2560, BLOCK), dt),
            pltpu.VMEM((2, BLOCK, 2048), dt),
            pltpu.VMEM((1024, 512), dt),
            pltpu.VMEM((1024, 512), dt),
            dma((4, 4, 4)), dma((16, 4)), dma((4, 2)), dma((8, 2)), dma((4, 2)), dma((4, 2)), dma((4,)),
            dma((10,)), dma((2,)), dma((4,)), dma((5,)),
        ],
        compiler_params=pltpu.CompilerParams(has_side_effects=True, vmem_limit_bytes=67043328),
        name="fused",
    )(low, side, grad)


def per_device(low, side, grad):
    right, lower, _ = fused(low, side, grad)
    row_pos = jnp.arange(lower.shape[0])[:, None]
    col_pos = jnp.arange(lower.shape[1])[None, :]
    row_global = (row_pos // BLOCK * 16 + lax.axis_index("row")) * BLOCK + row_pos % BLOCK
    col_global = (col_pos // BLOCK * 8 + lax.axis_index("col")) * BLOCK + col_pos % BLOCK
    return right, jnp.where(row_global >= col_global, lower, jnp.zeros_like(lower))


def solution(mesh):
    spec = P(("batch", "row"), "col")
    return jax.shard_map(per_device, mesh=mesh, in_specs=(spec,) * 3, out_specs=(spec,) * 2, check_vma=False)
```

```python
import jax
import jax.numpy as jnp
from jax import lax
from jax.experimental import pallas as pl
from jax.experimental.pallas import tpu as pltpu
from jax.sharding import PartitionSpec as P

BLOCK = 256
MESH = pl.DeviceIdType.MESH
NROWS = (1024, 768, 512, 256)
FIRST = (0, 1024, 1792, 2304)
ORDER = (3, 1, 0, 2)
SLACK = 0.0
QROWS = (256, 256, 256, 256)
QFIRST = (0, 256, 512, 768)
LINE = (0.0, 0.0)
LAG = 2.5


def plan():
    ready, jobs, steps = {}, [], []

    def job(need, link, cost, made, prio, step):
        jobs.append((need, link, cost, made, prio, step))

    for q in range(4):
        first = 1 if q < 2 else 0
        cost = 11.3 * QROWS[q] / 512
        def hop(off, axis, d):
            moved = list(off)
            moved[axis] = (moved[axis] - d) % 4
            return tuple(moved)
        ready[("mid", q)] = 16.0 + 8.0 * q
        job(("mid", q), "spread", 8.0, ("side", (0, 0), q), 0, ("spread", q))
        job(("mid", q), "a", 2.8, ("spread a", q), 0, ("none",))
        job(("mid", q), "b", 2.8, ("spread b", q), 0, ("none",))
        for lane in (None, 0, 1, 3, 2):
            axis = first if lane is None else 1 - first
            own = [0, 0]
            if lane is not None:
                own[first] = lane
            own = tuple(own)
            prio = 1 if lane is None else 5
            for d in (1, -1):
                job(("side", own, q), ("zy"[axis], d), cost, ("side", hop(own, axis, d), q), prio, ("side", own, q, axis, d))
            d = 1 if q % 2 == 0 else -1
            near = hop(own, axis, d)
            job(("side", near, q), ("zy"[axis], d), cost, ("side", hop(near, axis, d), q), prio, ("side", near, q, axis, d))
    for half in (1, 0):
        ready[("grad", 0, half)] = 0.0
        ready[("line", "own", half)] = LINE[half]
        for d in (1, -1):
            job(("grad", 0, half), ("z", d), 11.3, ("grad", -d % 4, half), 2 if half == 0 else 1, ("grad", 0, half, d))
        d = 1 if half == 0 else -1
        job(("grad", -d % 4, half), ("z", d), 11.3, ("grad", 2, half), 2 if half == 0 else 1, ("grad", -d % 4, half, d))
        for to in "ab":
            job(("line", "own", half), to, 11.3, ("line", to, half), 1, ("line", "own", half, to))
        job(("late", "a", half), "b", 11.3, ("line", "o", half), 4, ("line", "a", half, "b"))
        ready[("late", "a", half)] = (130.0, 130.0)[half]
        for piece in ("own", "a", "b", "o"):
            job(("line", piece, half), "sib", 1.0, ("line", piece + "s", half), 4, ("line", piece, half, "sib"))
    ready[("move", ORDER[0])] = 0.0
    ready[("hub", "end", 0)] = 0.0
    for n, kb in enumerate(ORDER):
        cost = 11.3 * NROWS[kb] / 1024
        for d in (1, -1):
            job(("move", kb), ("z", d), 1.5 * cost, ("move", (ORDER + ("end",))[n + 1]) if d == 1 else ("moved", kb), (0, 0, 0.5, 1.5)[n], ("move", kb, d))
        for zz in range(4):
            job(("hub", kb, zz), "b", cost, ("p", kb, zz), 2 + 0.1 * n, ("hub", kb, zz))
            job(("p", kb, zz), "a", cost, ("q", kb, zz), 2 + 0.1 * n, ("p", kb, zz))
            job(("q", kb, zz), "sib", 0.1 * cost, ("qs", kb, zz), 2, ("q", kb, zz))
        ready[("hub", kb, 0)] = 6.0 + 2 * n
        steps.append((2.0 + 2 * n, n, ("send", "stage", kb)))
    steps.append((28.0, 0, ("send", "zero")))
    free = {}
    pending = list(jobs)
    while pending:
        best = min((j for j in pending if j[0] in ready),
                   key=lambda j: (max(ready[j[0]], free.get(j[1], 0.0)), j[4], ready[j[0]]))
        pending.remove(best)
        need, link, cost, made, prio, step = best
        start = max(ready[need], free.get(link, 0.0))
        free[link] = start + cost
        ready[made] = start + cost + LAG
        if made[0] == "move":
            ready[made] = start + cost
            for zz, extra in ((1, 0.0), (3, 0.0), (2, cost / 3)):
                ready[("hub", step[1], zz)] = start + cost + LAG + extra
        lazy = SLACK if step[0] == "side" and step[1] != (0, 0) else 0.0
        late = 0.0
        if step[0] == "line" and step[-1] == "sib":
            late = {"own": 0.0, "o": 1e4 + 11}.get(step[1], 0.0)
        steps.append((max(ready[need] + lazy, start - 4.0, late), start, ("send",) + step))
        for kb in ORDER:
            key = ("sum", kb)
            if key not in ready and all(("qs", kb, zz) in ready for zz in range(4)) and ("grad", 2, 1) in ready and (kb > 1 or ("grad", 2, 0) in ready):
                now = max(t for e, t in ready.items() if e[:2] == ("qs", kb) or e[0] == "grad" and (kb < 2 or e[2] == 1)) + 3.0
                ready[key] = now
                steps.append((now, now, ("part", kb)))
                for d in (1, -1):
                    pending.append((key, ("y", d), 5.65, ("hop", kb, d), 0, ("none",)))
                    pending.append((("hop", kb, d), ("y", d), 11.3, ("got", kb, d), 0, ("near", kb, d)))
    for g in range(4):
        steps.append((1e4 + (0, 10, 12, 13)[g], g, ("dot", ("own", "a", "b", "o")[g])))
    steps = [(1e4 + 5, b, s) if s[:3] == ("send", "near", ORDER[-1]) else (a, b, s) for a, b, s in steps]
    steps.sort(key=lambda t: (t[0], t[1]))
    return [s for _, _, s in steps], ready


def kernel(low_ref, side_ref, grad_ref, right_ref, lower_ref, low_all,
           side_all, grad_all, line_all, acc, part, hop, got, lbuf, stage, obuf, rbuf,
           mid, low_recv, side_recv, grad_recv, line_recv, hop_recv, got_recv, mid_recv, send_sem, lbuf_sem, stage_sem, out_sem):
    r, c = lax.axis_index("row"), lax.axis_index("col")
    z, y, x, core = r // 4, r % 4, c // 2, c % 2
    hub = x // 2 == z % 2
    xa, xb = x + 1 - 2 * (x % 2), 3 - x
    xh = jnp.where(hub, x, xb)

    def place(zz, yy, xx, cc):
        return {"row": zz * 4 + yy, "col": xx * 2 + cc}

    def remote(src, dst, send, recv, to):
        return pltpu.make_async_remote_copy(src, dst, send_sem.at[send], recv, device_id=to, device_id_type=MESH)

    def arrive(ref, sem):
        pltpu.make_async_copy(ref, ref, sem).wait()

    sib = place(z, y, x, 1 - core)
    up, down = place(z, (y + 1) % 4, x, core), place(z, (y + 3) % 4, x, core)

    def shift(sig, kk):
        return (sig + kk * (5 - 2 * sig)) % 4

    def spread_row(cj, cc):
        return 2 * shift((cc // 2 + 4 - cj // 2) % 4, cj % 2) + (cj + cc) % 2

    def spread_col(row8, cj):
        return 2 * ((cj // 2 + shift(row8 // 2, cj % 2)) % 4) + (cj + row8) % 2

    def spread_from(row8, cc):
        kk = (cc + row8) % 2
        return 2 * ((cc // 2 + 4 - shift(row8 // 2, kk)) % 4) + kk

    side_row = (r // 8) * 8 + spread_row(c, r % 8)
    side_col = spread_col(r % 8, c)
    stays, direct = side_row == r, c == r % 8

    def quarter(ref, q):
        return ref.at[pl.ds(QFIRST[q], QROWS[q])]

    def spread_first():
        @pl.when(jnp.logical_not(stays) & jnp.logical_not(direct))
        def _():
            for q in range(4):
                remote(quarter(side_ref, q), quarter(mid, q), 0, mid_recv.at[q], {"row": side_row, "col": c}).start()

        @pl.when(jnp.logical_not(stays) & direct)
        def _():
            for q in range(4):
                remote(quarter(side_ref, q), quarter(side_all.at[side_row], q), 0, side_recv.at[side_row, q],
                       {"row": side_row, "col": c}).start()

        @pl.when(stays & direct)
        def _():
            for q in range(4):
                pltpu.make_async_copy(quarter(side_ref, q), quarter(side_all.at[r], q), side_recv.at[r, q]).start()

    def spread(q):
        to = {"row": r, "col": side_col}

        @pl.when((side_col != c) & (side_col != r % 8))
        def _():
            arrive(quarter(mid, q), mid_recv.at[q])
            remote(quarter(mid, q), quarter(side_all.at[r], q), 9, side_recv.at[r, q], to).start()

        @pl.when((side_col != c) & (side_col == r % 8))
        def _():
            remote(quarter(side_ref, q), quarter(side_all.at[r], q), 9, side_recv.at[r, q], to).start()

    mine = 2 * (x % 2) + core

    def low_piece(h, kb):
        return low_ref.at[pl.ds(kb * BLOCK, NROWS[kb]), pl.ds(pl.multiple_of((2 * kb + h) * BLOCK, BLOCK), BLOCK)]

    def low_at(yy, zz, kb):
        return low_all.at[yy, zz, pl.ds(FIRST[kb], NROWS[kb])]

    def stage_at(kb):
        return stage.at[pl.ds(FIRST[kb], NROWS[kb])]

    here = z // 2

    @pl.when(hub)
    def _():
        for kb in ORDER:
            pltpu.make_async_copy(low_piece(here, kb), stage_at(kb), stage_sem.at[kb]).start()

    def move(kb):
        @pl.when(hub)
        def _():
            remote(low_piece(1 - here, kb), low_at(mine, z, kb), 1, low_recv.at[mine, z, kb],
                   place((z + 2) % 4, y, x, core)).start()

        @pl.when(jnp.logical_not(hub))
        def _():
            for h in range(2):
                remote(low_piece(h, kb), low_at(mine, z, kb), 1, low_recv.at[mine, z, kb],
                       place(x // 2 + 2 * h, y, x, core)).start()

    move(ORDER[0])
    move(ORDER[1])
    spread_first()

    own_grad = pltpu.make_async_copy(grad_ref, grad_all.at[z], out_sem.at[0])
    own_line = pltpu.make_async_copy(grad_ref, line_all.at[c], out_sem.at[1])
    own_grad.start()
    own_line.start()

    def put_stage(kb):
        @pl.when(hub)
        def _():
            pltpu.make_async_copy(low_piece(here, kb), stage_at(kb), stage_sem.at[kb]).wait()
            pltpu.make_async_copy(stage_at(kb), low_at(mine, z, kb), low_recv.at[mine, z, kb]).start()

    steps, ready = plan()
    waited = set()

    def line_slot(piece):
        xx = {"own": x, "a": xa, "b": xb, "o": (x + 2) % 4}[piece.rstrip("s")]
        return xx * 2 + (1 - core if piece.endswith("s") else core)

    def half_at(ref, slot, half):
        return ref.at[slot, pl.ds(half * 512, 512)]

    def wait(event):
        if event in waited:
            return
        waited.add(event)
        name = event[0]
        if name == "side":
            slot = ((z + event[1][0]) % 4) * 4 + (y + event[1][1]) % 4
            arrive(quarter(side_all.at[slot], event[2]), side_recv.at[slot, event[2]])
        elif name == "grad":
            slot = (z + event[1]) % 4
            arrive(half_at(grad_all, slot, event[2]), grad_recv.at[slot, event[2]])
        elif name == "line":
            slot = line_slot(event[1])
            arrive(half_at(line_all, slot, event[2]), line_recv.at[slot, event[2]])
        else:
            yy = 2 * (xh % 2 if name in ("p", "ps") else 1 - xh % 2) + (1 - core if name.endswith("s") else core)
            zz = (z + event[2]) % 4
            arrive(low_at(yy, zz, event[1]), low_recv.at[yy, zz, event[1]])

    def low_send(yy, zz, kb, send, to):
        remote(low_at(yy, zz, kb), low_at(yy, zz, kb), send, low_recv.at[yy, zz, kb], to).start()

    def send(step):
        name = step[0]
        if name == "spread":
            spread(step[1])
        elif name == "stage":
            put_stage(step[1])
        elif name == "zero":
            acc[...] = jnp.zeros_like(acc)
        elif name == "move":
            if step[1] in ORDER[2:] and step[2] == 1:
                move(step[1])
        elif name == "side":
            _, off, q, axis, d = step
            wait(("side", off, q))
            slot = ((z + off[0]) % 4) * 4 + (y + off[1]) % 4
            to = place((z + d + 4) % 4, y, x, core) if axis == 0 else place(z, (y + d + 4) % 4, x, core)
            ref = quarter(side_all.at[slot], q)
            remote(ref, ref, 2, side_recv.at[slot, q], to).start()
        elif name == "grad":
            _, off, half, d = step
            if off:
                wait(("grad", off, half))
            slot = (z + off) % 4
            src = half_at(grad_all, slot, half) if off else grad_ref.at[pl.ds(half * 512, 512)]
            remote(src, half_at(grad_all, slot, half), 3, grad_recv.at[slot, half], place((z + d + 4) % 4, y, x, core)).start()
        elif name == "line":
            _, piece, half, to = step
            if piece != "own":
                wait(("line", piece, half))
            slot = line_slot(piece)
            src = half_at(line_all, slot, half) if piece != "own" else grad_ref.at[pl.ds(half * 512, 512)]
            dest = {"a": place(z, y, xa, core), "b": place(z, y, xb, core), "sib": sib}[to]
            remote(src, half_at(line_all, slot, half), 4, line_recv.at[slot, half], dest).start()
        elif name == "hub":
            _, kb, dz = step
            zz = (z + dz) % 4

            @pl.when(hub)
            def _():
                yy = mine
                arrive(low_at(yy, zz, kb), low_recv.at[yy, zz, kb])
                low_send(yy, zz, kb, 5, place(z, y, xb, core))
                low_send(yy, zz, kb, 5, place(z, y, xa, core))
                low_send(yy, zz, kb, 6, sib)
        elif name == "p":
            _, kb, dz = step
            zz = (z + dz) % 4
            yy = 2 * (xb % 2) + core

            @pl.when(jnp.logical_not(hub))
            def _():
                arrive(low_at(yy, zz, kb), low_recv.at[yy, zz, kb])
                low_send(yy, zz, kb, 5, place(z, y, xa, core))
                low_send(yy, zz, kb, 6, sib)
        elif name == "q":
            _, kb, dz = step
            zz = (z + dz) % 4
            wait(("q", kb, dz))
            low_send(2 * (1 - xh % 2) + core, zz, kb, 6, sib)
        elif name == "far":
            _, kb, d = step
            i = 0 if d == 1 else 1
            rows = pl.ds(i * 128, 128)
            remote(part.at[kb, 0, rows], hop.at[kb, i], 7, hop_recv.at[kb, i], up if d == 1 else down).start()
        elif name == "near":
            _, kb, d = step
            i, t = (0, 3) if d == 1 else (1, 1)
            arrive(hop.at[kb, i], hop_recv.at[kb, i])
            rows = pl.ds(i * 128, 128)
            part[kb, t, rows] += hop[kb, i]
            remote(part.at[kb, t], got.at[kb, i], 8, got_recv.at[kb, i], up if d == 1 else down).start()

    def add_part(kb):
        for zz in range(4):
            for name in ("ps", "q", "qs"):
                wait((name, kb, zz))
        if kb == ORDER[0]:
            own_grad.wait()
        for off in (1, 2, 3):
            for half in (1,) if kb > 1 else (0, 1):
                wait(("grad", off, half))
        n = NROWS[kb]

        def load(t):
            return pltpu.make_async_copy(low_all.at[(y + 2 + t) % 4, :, pl.ds(FIRST[kb], n)],
                                         lbuf.at[t % 2, :, pl.ds(0, n)], lbuf_sem.at[t % 2])

        load(0).start()

        def body(t, carry):
            @pl.when(t < 3)
            def _():
                load(t + 1).start()
            load(t).wait()
            total = jnp.zeros((BLOCK, 512), jnp.float32)
            for zz in range(4):
                total += lax.dot_general(lbuf[t % 2, zz, pl.ds(0, n)], grad_all[zz, pl.ds(kb * BLOCK, n)],
                                         (((0,), (0,)), ((), ())), preferred_element_type=jnp.float32)
            part[kb, t] = total
            return carry

        body(0, 0)
        send(("far", kb, 1))
        send(("far", kb, -1))
        lax.fori_loop(1, 4, body, 0)

    def add_dot(piece, start):
        for name in (piece, piece + "s"):
            if name != "own":
                for half in range(2):
                    wait(("line", name, half))
        if start:
            own_line.wait()
            for a in range(4):
                for b in range(4):
                    for q in range(4):
                        wait(("side", (a, b), q))
        first = line_slot(piece) // 2

        def body(i, carry):
            cj = 2 * first + i % 2
            h = i // 2
            slot = 8 * h + spread_row(cj, c)
            for bi in range(4):
                n = (bi + 1) * BLOCK
                total = lax.dot_general(line_all[cj, bi * BLOCK:(bi + 1) * BLOCK], side_all[slot, :n],
                                        (((1,), (1,)), ((), ())), preferred_element_type=jnp.float32)
                acc[h, bi, :, :n] += total
            return carry

        lax.fori_loop(0, 4, body, 0)

    started = False
    for step in steps:
        if step[0] == "send":
            send(step[1:])
        elif step[0] == "part":
            add_part(step[1])
        else:
            add_dot(step[1], not started)
            started = True

    for bi in range(4):
        if bi >= 2:
            pltpu.make_async_copy(obuf.at[bi % 2], lower_ref.at[pl.ds((bi - 2) * BLOCK, BLOCK)], out_sem.at[2 + bi % 2]).wait()
        for kb in range(4):
            for h in range(2):
                cols = pl.ds((2 * kb + h) * BLOCK, BLOCK)
                if kb <= bi:
                    obuf[bi % 2, :, cols] = acc[h, bi, :, kb * BLOCK:(kb + 1) * BLOCK].astype(jnp.bfloat16)
                else:
                    obuf[bi % 2, :, cols] = jnp.zeros((BLOCK, BLOCK), jnp.bfloat16)
        pltpu.make_async_copy(obuf.at[bi % 2], lower_ref.at[pl.ds(bi * BLOCK, BLOCK)], out_sem.at[2 + bi % 2]).start()
    for kb in range(4):
        for i in range(2):
            arrive(got.at[kb, i], got_recv.at[kb, i])
        rbuf[kb * BLOCK:(kb + 1) * BLOCK] = (part[kb, 2] + got[kb, 0] + got[kb, 1]).astype(jnp.bfloat16)
    out = pltpu.make_async_copy(rbuf, right_ref, out_sem.at[4])
    out.start()

    def sent(ref, i):
        pltpu.make_async_copy(ref, ref, send_sem.at[i]).wait()

    def pieces(n):
        return low_all.at[pl.ds(0, n // 4)] if n >= 4 else low_all.at[0, pl.ds(0, n)]

    @pl.when(jnp.logical_not(stays))
    def _():
        sent(side_all.at[0], 0)

    @pl.when(side_col != c)
    def _():
        sent(side_all.at[0], 9)

    @pl.when(hub)
    def _():
        sent(pieces(1), 1)
        sent(pieces(8), 5)

    @pl.when(jnp.logical_not(hub))
    def _():
        sent(pieces(2), 1)
        sent(pieces(4), 5)

    sent(side_all.at[pl.ds(0, 15)], 2)
    sent(grad_all.at[pl.ds(0, 3)], 3)
    sent(line_all.at[pl.ds(0, 7)], 4)
    sent(pieces(8), 6)
    sent(part.at[:, 0], 7)
    sent(got, 8)
    for bi in (2, 3):
        pltpu.make_async_copy(obuf.at[bi % 2], lower_ref.at[pl.ds(bi * BLOCK, BLOCK)], out_sem.at[2 + bi % 2]).wait()
    out.wait()


def fused(low, side, grad):
    dt = low.dtype
    f32 = jnp.float32
    anywhere = pl.BlockSpec(memory_space=pl.ANY)
    dma = pltpu.SemaphoreType.DMA
    return pl.pallas_call(
        kernel,
        out_shape=[jax.ShapeDtypeStruct(grad.shape, dt), jax.ShapeDtypeStruct(low.shape, dt),
                   jax.ShapeDtypeStruct((4, 4, 2560, BLOCK), dt)],
        in_specs=[anywhere] * 3,
        out_specs=[anywhere] * 3,
        scratch_shapes=[
            pltpu.VMEM((16, 1024, 512), dt),
            pltpu.VMEM((4, 1024, 512), dt),
            pltpu.VMEM((8, 1024, 512), dt),
            pltpu.VMEM((2, 4, BLOCK, 1024), f32),
            pltpu.VMEM((4, 4, BLOCK, 512), f32),
            pltpu.VMEM((4, 2, 128, 512), f32),
            pltpu.VMEM((4, 2, BLOCK, 512), f32),
            pltpu.VMEM((2, 4, 1024, BLOCK), dt),
            pltpu.VMEM((2560, BLOCK), dt),
            pltpu.VMEM((2, BLOCK, 2048), dt),
            pltpu.VMEM((1024, 512), dt),
            pltpu.VMEM((1024, 512), dt),
            dma((4, 4, 4)), dma((16, 4)), dma((4, 2)), dma((8, 2)), dma((4, 2)), dma((4, 2)), dma((4,)),
            dma((10,)), dma((2,)), dma((4,)), dma((5,)),
        ],
        compiler_params=pltpu.CompilerParams(has_side_effects=True, vmem_limit_bytes=67043328),
        name="fused",
    )(low, side, grad)


def per_device(low, side, grad):
    right, lower, _ = fused(low, side, grad)
    row_pos = jnp.arange(lower.shape[0])[:, None]
    col_pos = jnp.arange(lower.shape[1])[None, :]
    row_global = (row_pos // BLOCK * 16 + lax.axis_index("row")) * BLOCK + row_pos % BLOCK
    col_global = (col_pos // BLOCK * 8 + lax.axis_index("col")) * BLOCK + col_pos % BLOCK
    return right, jnp.where(row_global >= col_global, lower, jnp.zeros_like(lower))


def solution(mesh):
    spec = P(("batch", "row"), "col")
    return jax.shard_map(per_device, mesh=mesh, in_specs=(spec,) * 3, out_specs=(spec,) * 2, check_vma=False)
```
